64 devices in a mesh: data: 4 (over x, y), stage: 16 (over z, core).
Axes of the slice: x: 2, y: 2, z: 8, core: 2. Of those that a mesh axis runs over, the one named last changes fastest.
The devices are a block of a 4x4x8 slice.
Arguments:
- x_enc: bfloat16 [256, 512, 2048], P(('data', 'stage')), parts along dimension 0
- enc_len: int32 [256], P(('data', 'stage')), parts along dimension 0
- y: bfloat16 [256, 192, 2048], P(('data', 'stage')), parts along dimension 0
- enc_wqkv: bfloat16 [2, 2048, 3, 16, 128], replicated
- enc_wo: bfloat16 [2, 16, 128, 2048], replicated
- enc_w1: bfloat16 [2, 2048, 6144], replicated
- enc_w2: bfloat16 [2, 6144, 2048], replicated
- dec_wqkv: bfloat16 [2, 2048, 3, 16, 128], replicated
- dec_wo: bfloat16 [2, 16, 128, 2048], replicated
- cross_wq: bfloat16 [2, 2048, 8, 2, 128], replicated
- cross_wkv: bfloat16 [2, 2048, 2, 8, 128], replicated
- cross_wo: bfloat16 [2, 8, 2, 128, 2048], replicated
- dec_w1: bfloat16 [2, 2048, 6144], replicated
- dec_w2: bfloat16 [2, 6144, 2048], replicated
Outputs:
- output: bfloat16 [256, 192, 2048], P(('data', 'stage')), parts along dimension 0
There are 4 independent parts. The reference program is written for one: setup_inputs(seed, part) draws one part's arguments, and reference() takes and returns one part's arrays. A program takes and returns all parts, laid end to end along the dimension named above; an argument that names none is the same for every part.
All inputs are finite; a program needn't handle non-finite values.
Results may differ from the reference program's by a relative error of at most 0.0114466.
Values are sent between devices in bfloat16 or wider.
A program may use at most 768 MiB of HBM per device.

```python
import jax
import jax.numpy as jnp
from jax import lax

D = 2048
HEADS = 16
KV_HEADS = 8
HEAD = 128
FF = 6144
S_ENC = 512
S_DEC = 192
N_SEQ = 64
L_ENC = 2
L_DEC = 2

REP = HEADS // KV_HEADS


def weight(weight_key, shape, fan_in):
    return (jax.random.normal(weight_key, shape, jnp.float32) * fan_in ** -0.5).astype(jnp.bfloat16)


def structured(key_set, length):
    trend = jnp.linspace(-1.0, 1.0, length)[None, :, None]
    common = jax.random.normal(key_set[0], (N_SEQ, 1, D), jnp.float32)
    slope = jax.random.normal(key_set[1], (N_SEQ, 1, D), jnp.float32)
    noise = jax.random.normal(key_set[2], (N_SEQ, length, D), jnp.float32)
    return (0.5 * common + 0.8 * trend * slope + 0.4 * noise).astype(jnp.bfloat16)


def setup_inputs(seed: int = 0, part: int = 0) -> dict:
    part_keys = jax.random.split(jax.random.fold_in(jax.random.key(seed), part), 7)
    weight_keys = jax.random.split(jax.random.key(seed + 1), 11)
    lengths = jax.random.randint(part_keys[6], (N_SEQ,), S_ENC // 4, S_ENC + 1, jnp.int32)
    lengths = lengths.at[0].set(S_ENC)
    return {
        "x_enc": structured(part_keys[0:3], S_ENC),
        "enc_len": lengths,
        "y": structured(part_keys[3:6], S_DEC),
        "enc_wqkv": weight(weight_keys[0], (L_ENC, D, 3, HEADS, HEAD), D),
        "enc_wo": weight(weight_keys[1], (L_ENC, HEADS, HEAD, D), HEADS * HEAD),
        "enc_w1": weight(weight_keys[2], (L_ENC, D, FF), D),
        "enc_w2": weight(weight_keys[3], (L_ENC, FF, D), FF),
        "dec_wqkv": weight(weight_keys[4], (L_DEC, D, 3, HEADS, HEAD), D),
        "dec_wo": weight(weight_keys[5], (L_DEC, HEADS, HEAD, D), HEADS * HEAD),
        "cross_wq": weight(weight_keys[6], (L_DEC, D, KV_HEADS, REP, HEAD), D),
        "cross_wkv": weight(weight_keys[7], (L_DEC, D, 2, KV_HEADS, HEAD), D),
        "cross_wo": weight(weight_keys[8], (L_DEC, KV_HEADS, REP, HEAD, D), HEADS * HEAD),
        "dec_w1": weight(weight_keys[9], (L_DEC, D, FF), D),
        "dec_w2": weight(weight_keys[10], (L_DEC, FF, D), FF),
    }


def rms_norm(inputs):
    wide = inputs.astype(jnp.float32)
    return (wide * lax.rsqrt(jnp.mean(wide * wide, axis=-1, keepdims=True) + 1e-6)).astype(jnp.bfloat16)


def attend(query, keys, values, valid):
    scores = jnp.einsum("qgrd,kgd->grqk", query.astype(jnp.float32), keys.astype(jnp.float32)) * HEAD ** -0.5
    attn_probs = jax.nn.softmax(jnp.where(valid, scores, -1e30), axis=-1).astype(jnp.bfloat16)
    return jnp.einsum("grqk,kgd->qgrd", attn_probs.astype(jnp.float32), values.astype(jnp.float32)).astype(jnp.bfloat16)


def self_block(state, w_qkv, w_out, valid):
    proj_qkv = jnp.einsum("sd,dthe->tshe", rms_norm(state).astype(jnp.float32), w_qkv.astype(jnp.float32)).astype(jnp.bfloat16)
    mixed = attend(proj_qkv[0][:, :, None, :], proj_qkv[1], proj_qkv[2], valid)
    update = jnp.einsum("shre,hev->sv", mixed.astype(jnp.float32), w_out.astype(jnp.float32))
    return (state.astype(jnp.float32) + update).astype(jnp.bfloat16)


def ffn_block(state, w_in, w_out):
    hidden = jax.nn.gelu(jnp.dot(rms_norm(state), w_in, preferred_element_type=jnp.float32)).astype(jnp.bfloat16)
    return (state.astype(jnp.float32) + jnp.dot(hidden, w_out, preferred_element_type=jnp.float32)).astype(jnp.bfloat16)


def reference(x_enc, enc_len, y, enc_wqkv, enc_wo, enc_w1, enc_w2, dec_wqkv, dec_wo, cross_wq, cross_wkv, cross_wo, dec_w1, dec_w2):
    def encode_one(pair):
        state = pair[0]
        valid = jnp.arange(S_ENC) < pair[1]
        for layer in range(L_ENC):
            state = self_block(state, enc_wqkv[layer], enc_wo[layer], valid)
            state = ffn_block(state, enc_w1[layer], enc_w2[layer])
        return rms_norm(state)

    enc_states = lax.map(encode_one, (x_enc, enc_len))
    partner_out = jnp.roll(enc_states, N_SEQ // 2, axis=0)
    partner_len = jnp.roll(enc_len, N_SEQ // 2, axis=0)
    positions = jnp.arange(S_DEC)
    causal = positions[None, :] <= positions[:, None]

    def decode_one(triple):
        state, enc_seq, length = triple
        keep = jnp.arange(S_ENC) < length
        for layer in range(L_DEC):
            state = self_block(state, dec_wqkv[layer], dec_wo[layer], causal)
            query = jnp.einsum("sd,dgre->sgre", rms_norm(state).astype(jnp.float32), cross_wq[layer].astype(jnp.float32)).astype(jnp.bfloat16)
            key_vals = jnp.einsum("sd,dtge->tsge", enc_seq.astype(jnp.float32), cross_wkv[layer].astype(jnp.float32)).astype(jnp.bfloat16)
            mixed = attend(query, key_vals[0], key_vals[1], keep)
            update = jnp.einsum("sgre,grev->sv", mixed.astype(jnp.float32), cross_wo[layer].astype(jnp.float32))
            state = (state.astype(jnp.float32) + update).astype(jnp.bfloat16)
            state = ffn_block(state, dec_w1[layer], dec_w2[layer])
        return state

    return lax.map(decode_one, (y, partner_out, partner_len))
```

```python
import functools

import jax
import jax.numpy as jnp
from jax import lax
from jax.experimental import pallas as pl
from jax.experimental.pallas import tpu as pltpu
from jax.sharding import PartitionSpec as P

HEAD = 128
EPS = 1e-6
LOG2E = 1.4426950408889634
F32 = jnp.float32
BF16 = jnp.bfloat16
VMEM_LIMIT = 67043328


def dot(a, b):
    return jnp.dot(a, b, preferred_element_type=F32)


def dot_t(a, b):
    return lax.dot_general(a, b, (((1,), (1,)), ((), ())), preferred_element_type=F32)


def gelu(x):
    k = 0.7978845608028654
    half = 0.5 * x
    return half + half * jnp.tanh(x * (k + (k * 0.044715) * (x * x)))


def softmax_rows(scores, scale):
    top = jnp.max(scores, axis=-1, keepdims=True)
    weight = jnp.exp2((scores - top) * (scale * LOG2E))
    total = jnp.sum(weight, axis=-1, keepdims=True)
    return (weight * (1.0 / total)).astype(BF16)


def norm_rows(src, dst, rows, chunk):
    depth = src.shape[1]

    def step(i, _):
        at = pl.ds(pl.multiple_of(i * chunk, chunk), chunk)
        wide = src[at, :].astype(F32)
        mean = jnp.sum(wide * wide, axis=-1, keepdims=True) * (1.0 / depth)
        dst[at, :] = (wide * lax.rsqrt(mean + EPS)).astype(BF16)
        return 0

    lax.fori_loop(0, rows // chunk, step, 0)


def attend_units(count, make_scores, scale, finish):
    ahead = make_scores(0)
    for i in range(count):
        now = ahead
        if i + 1 < count:
            ahead = make_scores(i + 1)
        finish(i, softmax_rows(now, scale))


class Tiles:
    def __init__(self, buf, sem, group, sources):
        self.buf, self.sem, self.group, self.sources = buf, sem, group, sources

    def _copies(self, base, source, layer):
        refs = source(layer)
        return [
            pltpu.make_async_copy(ref, self.buf.at[base + k], self.sem.at[base + k])
            for k, ref in enumerate(refs)
        ]

    def start(self, base, source, layer):
        for copy in self._copies(base, source, layer):
            copy.start()

    def wait(self, base, source, layer):
        for copy in self._copies(base, source, layer):
            copy.wait()


def at_cols(i, width):
    return pl.ds(pl.multiple_of(i * width, width), width)


def cost(flops, bytes_accessed):
    return pl.CostEstimate(flops=int(flops), bytes_accessed=int(bytes_accessed), transcendentals=0)


def encoder_kernel(first_row, seqs, span, len_ref, x_ref, wqkv, wo, w1, w2, out_ref, h, xn, big, raw, ring, io_sem, raw_sem, ring_sem):
    layers, depth = wqkv.shape[0], wqkv.shape[1]
    heads = wqkv.shape[3]
    rows = seqs * span
    tile = depth // 2
    tile_heads = tile // HEAD
    piece = min(512, tile)
    n_qkv = 6
    scale = HEAD**-0.5

    raws = Tiles(raw, raw_sem, 1, None)
    plain = Tiles(ring, ring_sem, 3, None)

    def qkv_src(u):
        layer, j = u // n_qkv, lax.rem(u, n_qkv)
        return lambda _: [wqkv.at[layer, :, j // 2, pl.ds(pl.multiple_of(lax.rem(j, 2) * tile_heads, tile_heads), tile_heads), :]]

    def wo_src(layer):
        return [wo.at[layer, :, pl.ds(n * tile, tile)] for n in range(2)]

    def w1_src(t):
        return lambda layer: [w1.at[layer, :, at_cols(t * 3 + k, tile)] for k in range(3)]

    def w2_src(t):
        return lambda layer: [w2.at[layer, pl.ds(k * depth, depth), at_cols(t, tile)] for k in range(3)]

    load = pltpu.make_async_copy(x_ref.at[pl.ds(first_row, rows), :], h, io_sem)
    load.start()
    raws.start(0, qkv_src(0), 0)
    raws.start(1, qkv_src(1), 0)
    plain.start(0, wo_src, 0)
    load.wait()

    def layer_step(layer, _):
        def base_of(g):
            return lax.rem(5 * layer + g, 2) * 3

        norm_rows(h, xn, rows, 128)

        def qkv_step(j, _):
            u = layer * n_qkv + j
            slot = lax.rem(u, 3)
            raws.wait(slot, qkv_src(u), 0)

            @pl.when(u + 2 < layers * n_qkv)
            def _():
                raws.start(lax.rem(u + 2, 3), qkv_src(u + 2), 0)

            w = raw[slot].reshape(depth, tile)
            for n in range(tile // piece):
                big[:, pl.ds(pl.multiple_of(j * tile + n * piece, piece), piece)] = dot(xn[...], w[:, n * piece : (n + 1) * piece]).astype(BF16)
            return 0

        lax.fori_loop(0, n_qkv, qkv_step, 0)

        per_trip = tile_heads

        def attend_step(i, _):
            b, g = i // (heads // per_trip), lax.rem(i, heads // per_trip)
            keep = lax.broadcasted_iota(jnp.int32, (1, span), 1) < len_ref[b + first_row // span]
            at = pl.ds(pl.multiple_of(b * span, span), span)

            def col(u, which):
                return pl.ds(pl.multiple_of(which * depth + (g * per_trip + u) * HEAD, HEAD), HEAD)

            def scores(u):
                return jnp.where(keep, dot_t(big[at, col(u, 0)], big[at, col(u, 1)]), -1e30 / scale)

            def finish(u, probs):
                xn[at, col(u, 0)] = dot(probs, big[at, col(u, 2)]).astype(BF16)

            attend_units(per_trip, scores, scale, finish)
            return 0

        lax.fori_loop(0, seqs * (heads // per_trip), attend_step, 0)

        base = base_of(0)
        plain.wait(base, wo_src, layer)
        plain.start(base_of(1), w1_src(0), layer)
        for n in range(depth // piece):
            cols = slice(n * piece, (n + 1) * piece)
            w = ring[base + n * piece // tile, :, (n * piece) % tile : (n * piece) % tile + piece]
            h[:, cols] = (h[:, cols].astype(F32) + dot(xn[...], w)).astype(BF16)

        norm_rows(h, xn, rows, 128)

        def w1_step(t, _):
            base = base_of(1 + t)
            plain.wait(base, w1_src(t), layer)

            @pl.when(t == 0)
            def _():
                plain.start(base_of(2), w1_src(1), layer)

            @pl.when(t == 1)
            def _():
                plain.start(base_of(3), w2_src(0), layer)

            for k in range(3):
                for n in range(tile // piece):
                    w = ring[base + k, :, n * piece : (n + 1) * piece]
                    big[:, pl.ds(pl.multiple_of((t * 3 + k) * tile + n * piece, piece), piece)] = gelu(dot(xn[...], w)).astype(BF16)
            return 0

        lax.fori_loop(0, 2, w1_step, 0)

        def w2_step(t, _):
            base = base_of(3 + t)
            plain.wait(base, w2_src(t), layer)

            @pl.when(t == 0)
            def _():
                plain.start(base_of(4), w2_src(1), layer)

            @pl.when(jnp.logical_and(t == 1, layer + 1 < layers))
            def _():
                plain.start(base_of(5), wo_src, layer + 1)

            for n in range(tile // piece):
                total = None
                for k in range(3):
                    part = dot(big[:, k * depth : (k + 1) * depth], ring[base + k, :, n * piece : (n + 1) * piece])
                    total = part if total is None else total + part
                cols = pl.ds(pl.multiple_of(t * tile + n * piece, piece), piece)
                h[:, cols] = (h[:, cols].astype(F32) + total).astype(BF16)
            return 0

        lax.fori_loop(0, 2, w2_step, 0)
        return 0

    lax.fori_loop(0, layers, layer_step, 0)
    norm_rows(h, xn, rows, 128)
    store = pltpu.make_async_copy(xn, out_ref, io_sem)
    store.start()
    store.wait()


def encoder_call(first_seq, seqs, x, enc_len, wqkv, wo, w1, w2):
    span, depth = x.shape[1], x.shape[2]
    layers, ff = wqkv.shape[0], w1.shape[2]
    rows, tile = seqs * span, depth // 2
    heads = wqkv.shape[3]
    assert ff == 3 * depth and heads * HEAD == depth
    any_spec = pl.BlockSpec(memory_space=pl.ANY)
    per_layer = 2 * rows * depth * (4 * depth + 2 * ff) + 4 * seqs * heads * span * span * HEAD
    return pl.pallas_call(
        functools.partial(encoder_kernel, first_seq * span, seqs, span),
        out_shape=jax.ShapeDtypeStruct((rows, depth), BF16),
        in_specs=[pl.BlockSpec(memory_space=pltpu.SMEM)] + [any_spec] * 5,
        out_specs=any_spec,
        scratch_shapes=[
            pltpu.VMEM((rows, depth), BF16),
            pltpu.VMEM((rows, depth), BF16),
            pltpu.VMEM((rows, ff), BF16),
            pltpu.VMEM((3, depth, tile // HEAD, HEAD), BF16),
            pltpu.VMEM((6, depth, tile), BF16),
            pltpu.SemaphoreType.DMA,
            pltpu.SemaphoreType.DMA((3,)),
            pltpu.SemaphoreType.DMA((6,)),
        ],
        compiler_params=pltpu.CompilerParams(vmem_limit_bytes=VMEM_LIMIT),
        cost_estimate=cost(layers * per_layer, 2 * layers * depth * (4 * depth + 2 * ff)),
        name="encode",
    )(enc_len, x.reshape(-1, depth), wqkv, wo.reshape(layers, depth, depth), w1, w2)


def decoder_kernel(first_row, first_len, seqs, span, len_ref, y_ref, enc_ref, wqkv, wo, wq, wkv, wc, w1, w2, out_ref, z, xn, big, enc, kv, raw, ring, io_sem, raw_sem, ring_sem):
    layers, depth = wqkv.shape[0], wqkv.shape[1]
    heads = wqkv.shape[3]
    kv_heads = wkv.shape[3]
    rep = heads // kv_heads
    rows = z.shape[0]
    ctx = enc.shape[0] // seqs
    tile = depth // 2
    tile_heads = tile // HEAD
    piece = min(512, tile)
    scale = HEAD**-0.5

    raws = Tiles(raw, raw_sem, 2, None)
    plain = Tiles(ring, ring_sem, 3, None)

    def half(n):
        return pl.ds(n * tile_heads, tile_heads)

    def qkv_src(t):
        return lambda layer: [wqkv.at[layer, :, t, half(n), :] for n in range(2)]

    def wq_src(layer):
        return [wq.at[layer, :, half(n), :] for n in range(2)]

    def wkv_src(layer):
        return [wkv.at[layer, :, n, :, :] for n in range(2)]

    def wo_src(layer):
        return [wo.at[layer, :, pl.ds(n * tile, tile)] for n in range(2)]

    def wc_src(layer):
        return [wc.at[layer, :, pl.ds(n * tile, tile)] for n in range(2)]

    def w1_src(t):
        return lambda layer: [w1.at[layer, :, at_cols(t * 3 + k, tile)] for k in range(3)]

    def w2_src(t):
        return lambda layer: [w2.at[layer, pl.ds(k * depth, depth), at_cols(t, tile)] for k in range(3)]

    load = pltpu.make_async_copy(y_ref.at[pl.ds(first_row, rows), :], z, io_sem.at[0])
    load.start()
    raws.start(0, qkv_src(0), 0)
    plain.start(0, wo_src, 0)
    load_enc = pltpu.make_async_copy(enc_ref, enc, io_sem.at[1])
    load_enc.start()
    load.wait()

    def project(dst, lhs, bases, place):
        for k, slot in enumerate(bases):
            w = raw[slot].reshape(depth, tile)
            for n in range(tile // piece):
                dst[:, place(k * tile + n * piece)] = dot(lhs[...], w[:, n * piece : (n + 1) * piece]).astype(BF16)

    def add_out(base):
        for n in range(depth // piece):
            cols = slice(n * piece, (n + 1) * piece)
            w = ring[base + n * piece // tile, :, (n * piece) % tile : (n * piece) % tile + piece]
            z[:, cols] = (z[:, cols].astype(F32) + dot(xn[...], w)).astype(BF16)

    def fixed(c):
        return pl.ds(c, piece)

    def layer_step(layer, _):
        def raw_base(g):
            return lax.rem(5 * layer + g, 2) * 2

        def base_of(g):
            return lax.rem(6 * layer + g, 2) * 3

        norm_rows(z, xn, rows, 64)

        def qkv_step(t, _):
            base = raw_base(t)
            raws.wait(base, qkv_src(t), layer)

            @pl.when(t < 2)
            def _():
                raws.start(raw_base(t + 1), qkv_src(t + 1), layer)

            @pl.when(t == 2)
            def _():
                raws.start(raw_base(3), wkv_src, layer)

            project(big, xn, (base, base + 1), lambda c: pl.ds(pl.multiple_of(t * depth + c, piece), piece))
            return 0

        lax.fori_loop(0, 3, qkv_step, 0)

        causal = lax.broadcasted_iota(jnp.int32, (span, span), 1) <= lax.broadcasted_iota(jnp.int32, (span, span), 0)

        def self_step(b, _):
            at = pl.ds(pl.multiple_of(b * span, span), span)

            def col(u, which):
                return pl.ds(which * depth + u * HEAD, HEAD)

            def scores(u):
                return jnp.where(causal, dot_t(big[at, col(u, 0)], big[at, col(u, 1)]), -1e30 / scale)

            def finish(u, probs):
                xn[at, col(u, 0)] = dot(probs, big[at, col(u, 2)]).astype(BF16)

            attend_units(heads, scores, scale, finish)
            return 0

        lax.fori_loop(0, seqs, self_step, 0)

        base = base_of(0)
        plain.wait(base, wo_src, layer)
        plain.start(base_of(1), wc_src, layer)
        add_out(base)

        @pl.when(layer == 0)
        def _():
            load_enc.wait()

        base = raw_base(3)
        raws.wait(base, wkv_src, layer)
        raws.start(raw_base(4), wq_src, layer)
        project(kv, enc, (base, base + 1), fixed)

        norm_rows(z, xn, rows, 64)
        base = raw_base(4)
        raws.wait(base, wq_src, layer)

        @pl.when(layer + 1 < layers)
        def _():
            raws.start(raw_base(5), qkv_src(0), layer + 1)

        project(big, xn, (base, base + 1), fixed)

        def cross_step(b, _):
            at = pl.ds(pl.multiple_of(b * span, span), span)
            at_kv = pl.ds(pl.multiple_of(b * ctx, ctx), ctx)
            keep = lax.broadcasted_iota(jnp.int32, (1, ctx), 1) < len_ref[b + first_len]

            def scores(g):
                query = jnp.concatenate([big[at, pl.ds((g * rep + r) * HEAD, HEAD)] for r in range(rep)], axis=0)
                return jnp.where(keep, dot_t(query, kv[at_kv, pl.ds(g * HEAD, HEAD)]), -1e30 / scale)

            def finish(g, probs):
                mixed = dot(probs, kv[at_kv, pl.ds((kv_heads + g) * HEAD, HEAD)]).astype(BF16)
                for r in range(rep):
                    xn[at, pl.ds((g * rep + r) * HEAD, HEAD)] = mixed[r * span : (r + 1) * span]

            attend_units(kv_heads, scores, scale, finish)
            return 0

        lax.fori_loop(0, seqs, cross_step, 0)

        base = base_of(1)
        plain.wait(base, wc_src, layer)
        plain.start(base_of(2), w1_src(0), layer)
        add_out(base)

        norm_rows(z, xn, rows, 64)

        def w1_step(t, _):
            base = base_of(2 + t)
            plain.wait(base, w1_src(t), layer)

            @pl.when(t == 0)
            def _():
                plain.start(base_of(3), w1_src(1), layer)

            @pl.when(t == 1)
            def _():
                plain.start(base_of(4), w2_src(0), layer)

            for k in range(3):
                for n in range(tile // piece):
                    w = ring[base + k, :, n * piece : (n + 1) * piece]
                    big[:, pl.ds(pl.multiple_of((t * 3 + k) * tile + n * piece, piece), piece)] = gelu(dot(xn[...], w)).astype(BF16)
            return 0

        lax.fori_loop(0, 2, w1_step, 0)

        def w2_step(t, _):
            base = base_of(4 + t)
            plain.wait(base, w2_src(t), layer)

            @pl.when(t == 0)
            def _():
                plain.start(base_of(5), w2_src(1), layer)

            @pl.when(jnp.logical_and(t == 1, layer + 1 < layers))
            def _():
                plain.start(base_of(6), wo_src, layer + 1)

            for n in range(tile // piece):
                total = None
                for k in range(3):
                    part = dot(big[:, k * depth : (k + 1) * depth], ring[base + k, :, n * piece : (n + 1) * piece])
                    total = part if total is None else total + part
                cols = pl.ds(pl.multiple_of(t * tile + n * piece, piece), piece)
                z[:, cols] = (z[:, cols].astype(F32) + total).astype(BF16)
            return 0

        lax.fori_loop(0, 2, w2_step, 0)
        return 0

    lax.fori_loop(0, layers, layer_step, 0)
    store = pltpu.make_async_copy(z, out_ref, io_sem.at[0])
    store.start()
    store.wait()


def decoder_call(first_seq, seqs, y, first_len, enc_len, enc, wqkv, wo, wq, wkv, wc, w1, w2):
    span, depth = y.shape[1], y.shape[2]
    layers, ff = wqkv.shape[0], w1.shape[2]
    heads = wqkv.shape[3]
    rows, tile, ctx = seqs * span, depth // 2, enc.shape[0]
    assert ff == 3 * depth and heads * HEAD == depth
    any_spec = pl.BlockSpec(memory_space=pl.ANY)
    per_layer = 2 * rows * depth * (6 * depth + 2 * ff) + 4 * ctx * depth * depth + 4 * seqs * heads * span * (span + ctx // seqs) * HEAD
    return pl.pallas_call(
        functools.partial(decoder_kernel, first_seq * span, first_len, seqs, span),
        out_shape=jax.ShapeDtypeStruct((rows, depth), BF16),
        in_specs=[pl.BlockSpec(memory_space=pltpu.SMEM)] + [any_spec] * 9,
        out_specs=any_spec,
        scratch_shapes=[
            pltpu.VMEM((rows, depth), BF16),
            pltpu.VMEM((rows, depth), BF16),
            pltpu.VMEM((rows, ff), BF16),
            pltpu.VMEM((ctx, depth), BF16),
            pltpu.VMEM((ctx, depth), BF16),
            pltpu.VMEM((4, depth, tile // HEAD, HEAD), BF16),
            pltpu.VMEM((6, depth, tile), BF16),
            pltpu.SemaphoreType.DMA((2,)),
            pltpu.SemaphoreType.DMA((4,)),
            pltpu.SemaphoreType.DMA((6,)),
        ],
        compiler_params=pltpu.CompilerParams(vmem_limit_bytes=VMEM_LIMIT),
        cost_estimate=cost(layers * per_layer, 2 * layers * depth * (8 * depth + 2 * ff)),
        name="decode",
    )(
        enc_len,
        y.reshape(-1, depth),
        enc,
        wqkv,
        wo.reshape(layers, depth, depth),
        wq.reshape(layers, depth, heads, HEAD),
        wkv,
        wc.reshape(layers, depth, depth),
        w1,
        w2,
    )


def solution(mesh):
    stages = mesh.shape["stage"]
    swap = [(source, (source + stages // 2) % stages) for source in range(stages)]
    rows = P(("data", "stage"))
    whole = P()

    def body(x_enc, enc_len, y, enc_wqkv, enc_wo, enc_w1, enc_w2, dec_wqkv, dec_wo, cross_wq, cross_wkv, cross_wo, dec_w1, dec_w2):
        seqs, span, depth = y.shape
        half = seqs // 2
        enc_weights = (enc_wqkv, enc_wo, enc_w1, enc_w2)
        dec_weights = (dec_wqkv, dec_wo, cross_wq, cross_wkv, cross_wo, dec_w1, dec_w2)

        away_y = lax.ppermute(y[:half], "stage", swap)
        len_recv = lax.ppermute(enc_len, "stage", swap)
        home_enc = encoder_call(half, half, x_enc, enc_len, *enc_weights)
        home_recv = lax.ppermute(home_enc, "stage", swap)
        x_next, _ = lax.optimization_barrier((x_enc, home_enc))
        away_enc = encoder_call(0, half, x_next, enc_len, *enc_weights)
        away_out = decoder_call(0, half, away_y, 0, enc_len, away_enc, *dec_weights)
        out_recv = lax.ppermute(away_out, "stage", swap)
        y_next, _ = lax.optimization_barrier((y, away_out))
        home_out = decoder_call(half, half, y_next, half, len_recv, home_recv, *dec_weights)
        return jnp.concatenate([out_recv, home_out], axis=0).reshape(y.shape)

    return jax.shard_map(body, mesh=mesh, in_specs=(rows, rows, rows) + (whole,) * 11, out_specs=rows, check_vma=False)
```

```python
import functools

import jax
import jax.numpy as jnp
from jax import lax
from jax.experimental import pallas as pl
from jax.experimental.pallas import tpu as pltpu
from jax.sharding import PartitionSpec as P

HEAD = 128
LANES = 128
EPS = 1e-6
LOG2E = 1.4426950408889634
F32 = jnp.float32
BF16 = jnp.bfloat16
VMEM_LIMIT = 67043328


def dot(a, b):
    return jnp.dot(a, b, preferred_element_type=F32)


def dot_t(a, b):
    return lax.dot_general(a, b, (((1,), (1,)), ((), ())), preferred_element_type=F32)


def gelu(x):
    k = -2.0 * 0.7978845608028654 * LOG2E
    return x / (1.0 + jnp.exp2(x * (k + (k * 0.044715) * (x * x))))


def softmax_rows(scores, scale):
    top = jnp.max(scores, axis=-1, keepdims=True)
    weight = jnp.exp2((scores - top) * (scale * LOG2E))
    total = jnp.sum(weight, axis=-1, keepdims=True)
    return (weight * (1.0 / total)).astype(BF16)


def attend_units(count, make_scores, scale, finish):
    ahead = make_scores(0)
    for i in range(count):
        now = ahead
        if i + 1 < count:
            ahead = make_scores(i + 1)
        finish(i, softmax_rows(now, scale))


def joined(ref, blocks, rows=slice(None)):
    return jnp.concatenate([ref[c, rows] for c in blocks], axis=1)


def square_sum(ref, first, count):
    total = None
    for c in range(count):
        wide = ref[first + c].astype(F32)
        total = wide * wide if total is None else total + wide * wide
    return total


def settle_norm(sums, rstd, depth):
    mean = jnp.sum(sums[...], axis=-1, keepdims=True) * (1.0 / depth)
    rstd[...] = jnp.broadcast_to(lax.rsqrt(mean + EPS), rstd.shape)
    sums[...] = jnp.zeros_like(sums)


def normalize(state, rstd, dst):
    for c in range(state.shape[0]):
        dst[c] = (state[c].astype(F32) * rstd[...]).astype(BF16)


def add_to_state(state, sums, first, update):
    part = None
    for k in range(update.shape[1] // LANES):
        fresh = (state[first + k].astype(F32) + update[:, k * LANES : (k + 1) * LANES]).astype(BF16)
        state[first + k] = fresh
        wide = fresh.astype(F32)
        part = wide * wide if part is None else part + wide * wide
    sums[...] += part


def put_blocks(dst, first, value, rows=slice(None)):
    for k in range(value.shape[1] // LANES):
        dst[first + k, rows] = value[:, k * LANES : (k + 1) * LANES]


def block_copies(hbm, row0, buf, sems, to_hbm=False):
    blocks, rows = buf.shape[0], buf.shape[1]
    copies = []
    for c in range(blocks):
        there = hbm.at[pl.ds(row0, rows), pl.ds(c * LANES, LANES)]
        here = buf.at[c]
        copies.append(pltpu.make_async_copy(here, there, sems.at[c]) if to_hbm else pltpu.make_async_copy(there, here, sems.at[c]))
    return copies


class Ring:
    def __init__(self, buf, sem):
        self.buf, self.sem = buf, sem

    def copies(self, base, refs):
        return [pltpu.make_async_copy(ref, self.buf.at[base + k], self.sem.at[base + k]) for k, ref in enumerate(refs)]

    def start(self, base, refs):
        for copy in self.copies(base, refs):
            copy.start()

    def wait(self, base, refs):
        for copy in self.copies(base, refs):
            copy.wait()


def at_cols(i, width):
    return pl.ds(pl.multiple_of(i * width, width), width)


def loop(count, step):
    def body(i, carry):
        step(i)
        return carry

    lax.fori_loop(0, count, body, 0)


def load_state(copies, state, sums):
    for c, copy in enumerate(copies):
        copy.wait()
        part = square_sum(state, c, 1)
        if c == 0:
            sums[...] = part
        else:
            sums[...] += part


def ffn_in(xn, big, ring, base, t, tile, piece, row_piece):
    blocks = range(xn.shape[0])
    per = piece // LANES
    for k in range(3):
        for n in range(tile // piece):
            w = ring[base + k, :, n * piece : (n + 1) * piece]
            for m in range(xn.shape[1] // row_piece):
                rows = slice(m * row_piece, (m + 1) * row_piece)
                put_blocks(big, t * (3 * tile // LANES) + (k * tile + n * piece) // LANES, gelu(dot(joined(xn, blocks, rows), w)).astype(BF16), rows)


def ffn_out(state, sums, big, ring, base, t, tile, piece):
    depth_blocks = state.shape[0]
    for n in range(tile // piece):
        total = None
        for k in range(3):
            part = dot(joined(big, range(k * depth_blocks, (k + 1) * depth_blocks)), ring[base + k, :, n * piece : (n + 1) * piece])
            total = part if total is None else total + part
        add_to_state(state, sums, t * (tile // LANES) + n * piece // LANES, total)


def cost(flops, bytes_accessed):
    return pl.CostEstimate(flops=int(flops), bytes_accessed=int(bytes_accessed), transcendentals=0)


def encoder_kernel(first_row, seqs, span, len_ref, x_ref, wqkv, wo, w1, w2, out_ref, h, xn, big, sums, rstd, raw, ring_buf, io_sem, raw_sem, ring_sem):
    layers, depth = wqkv.shape[0], wqkv.shape[1]
    heads = wqkv.shape[3]
    rows = seqs * span
    tile = depth // 2
    tile_heads = tile // HEAD
    piece = min(512, tile)
    row_piece = min(512, rows)
    blocks = depth // LANES
    n_qkv = 6
    scale = HEAD**-0.5

    raws = Ring(raw, raw_sem)
    ring = Ring(ring_buf, ring_sem)

    def qkv_src(layer, j):
        return [wqkv.at[layer, :, j // 2, pl.ds(pl.multiple_of(lax.rem(j, 2) * tile_heads, tile_heads), tile_heads), :]]

    def wo_src(layer):
        return [wo.at[layer, :, pl.ds(n * tile, tile)] for n in range(2)]

    def w1_src(layer, t):
        return [w1.at[layer, :, pl.ds((t * 3 + k) * tile, tile)] for k in range(3)]

    def w2_src(layer, t):
        return [w2.at[layer, pl.ds(k * depth, depth), pl.ds(t * tile, tile)] for k in range(3)]

    load = block_copies(x_ref, first_row, h, io_sem)
    for copy in load:
        copy.start()
    raws.start(0, qkv_src(0, 0))
    load_state(load, h, sums)
    settle_norm(sums, rstd, depth)
    raws.start(1, qkv_src(0, 1))
    ring.start(0, wo_src(0))

    for layer in range(layers):
        last = layer + 1 == layers
        bases = [((5 * layer + g) % 2) * 3 for g in range(6)]

        def qkv_step(j):
            slot = lax.rem(j, 3)
            raws.wait(slot, qkv_src(layer, j))

            @pl.when(j < n_qkv - 2)
            def _():
                raws.start(lax.rem(j + 2, 3), qkv_src(layer, j + 2))

            if not last:

                @pl.when(j >= n_qkv - 2)
                def _():
                    raws.start(lax.rem(j + 2, 3), qkv_src(layer + 1, j + 2 - n_qkv))

            normalize(h, rstd, xn)
            w = raw[slot].reshape(depth, tile)
            for n in range(tile // piece):
                put_blocks(big, j * (tile // LANES) + n * piece // LANES, dot(joined(xn, range(blocks)), w[:, n * piece : (n + 1) * piece]).astype(BF16))

        loop(n_qkv, qkv_step)

        def attend_step(i):
            groups = heads // tile_heads
            b, g = i // groups, lax.rem(i, groups)
            keep = lax.broadcasted_iota(jnp.int32, (1, span), 1) < len_ref[b + first_row // span]
            at = pl.ds(pl.multiple_of(b * span, span), span)

            def head(u, which):
                return which * heads + g * tile_heads + u

            def scores(u):
                return jnp.where(keep, dot_t(big[head(u, 0), at], big[head(u, 1), at]), -1e30 / scale)

            def finish(u, probs):
                xn[head(u, 0), at] = dot(probs, big[head(u, 2), at]).astype(BF16)

            attend_units(tile_heads, scores, scale, finish)

        loop(seqs * (heads // tile_heads), attend_step)

        ring.wait(bases[0], wo_src(layer))
        ring.start(bases[1], w1_src(layer, 0))

        def wo_step(t):
            for n in range(tile // piece):
                add_to_state(h, sums, t * (tile // LANES) + n * piece // LANES, dot(joined(xn, range(blocks)), ring_buf[bases[0] + t, :, n * piece : (n + 1) * piece]))

        loop(2, wo_step)
        settle_norm(sums, rstd, depth)

        def w1_step(t):
            base = jnp.where(t == 0, bases[1], bases[2])
            ring.wait(base, w1_src(layer, 0))

            @pl.when(t == 0)
            def _():
                ring.start(bases[2], w1_src(layer, 1))

            @pl.when(t == 1)
            def _():
                ring.start(bases[3], w2_src(layer, 0))

            normalize(h, rstd, xn)
            ffn_in(xn, big, ring_buf, base, t, tile, piece, row_piece)

        loop(2, w1_step)

        def w2_step(t):
            base = jnp.where(t == 0, bases[3], bases[4])
            ring.wait(base, w2_src(layer, 0))

            @pl.when(t == 0)
            def _():
                ring.start(bases[4], w2_src(layer, 1))

            if not last:

                @pl.when(t == 1)
                def _():
                    ring.start(bases[5], wo_src(layer + 1))

            ffn_out(h, sums, big, ring_buf, base, t, tile, piece)

        loop(2, w2_step)
        settle_norm(sums, rstd, depth)

    normalize(h, rstd, xn)
    store = block_copies(out_ref, 0, xn, io_sem, to_hbm=True)
    for copy in store:
        copy.start()
    for copy in store:
        copy.wait()


def encoder_call(first_seq, seqs, x, enc_len, wqkv, wo, w1, w2):
    span, depth = x.shape[1], x.shape[2]
    layers, ff = wqkv.shape[0], w1.shape[2]
    rows, tile = seqs * span, depth // 2
    heads = wqkv.shape[3]
    assert ff == 3 * depth and heads * HEAD == depth
    any_spec = pl.BlockSpec(memory_space=pl.ANY)
    per_layer = 2 * rows * depth * (4 * depth + 2 * ff) + 4 * seqs * heads * span * span * HEAD
    return pl.pallas_call(
        functools.partial(encoder_kernel, first_seq * span, seqs, span),
        out_shape=jax.ShapeDtypeStruct((rows, depth), BF16),
        in_specs=[pl.BlockSpec(memory_space=pltpu.SMEM)] + [any_spec] * 5,
        out_specs=any_spec,
        scratch_shapes=[
            pltpu.VMEM((depth // LANES, rows, LANES), BF16),
            pltpu.VMEM((depth // LANES, rows, LANES), BF16),
            pltpu.VMEM((ff // LANES, rows, LANES), BF16),
            pltpu.VMEM((rows, LANES), F32),
            pltpu.VMEM((rows, LANES), F32),
            pltpu.VMEM((3, depth, tile // HEAD, HEAD), BF16),
            pltpu.VMEM((6, depth, tile), BF16),
            pltpu.SemaphoreType.DMA((depth // LANES,)),
            pltpu.SemaphoreType.DMA((3,)),
            pltpu.SemaphoreType.DMA((6,)),
        ],
        compiler_params=pltpu.CompilerParams(vmem_limit_bytes=VMEM_LIMIT),
        cost_estimate=cost(layers * per_layer, 2 * layers * depth * (4 * depth + 2 * ff)),
        name="encode",
    )(enc_len, x.reshape(-1, depth), wqkv, wo.reshape(layers, depth, depth), w1, w2)


def decoder_kernel(first_row, out_row, first_len, seqs, span, len_ref, y_ref, enc_ref, wqkv, wo, wq, wkv, wc, w1, w2, out_ref, z, xn, big, enc, kv, sums, rstd, raw, ring_buf, io_sem, enc_sem, raw_sem, ring_sem):
    layers, depth = wqkv.shape[0], wqkv.shape[1]
    heads = wqkv.shape[3]
    kv_heads = wkv.shape[3]
    rep = heads // kv_heads
    rows = z.shape[1]
    ctx = enc.shape[1] // seqs
    tile = depth // 2
    tile_heads = tile // HEAD
    piece = min(512, tile)
    blocks = depth // LANES
    scale = HEAD**-0.5

    raws = Ring(raw, raw_sem)
    ring = Ring(ring_buf, ring_sem)

    def raw_src(layer, idx):
        if isinstance(idx, int) and idx >= 10:
            return raw_src(layer + 1, idx - 10)
        if isinstance(idx, int) and idx >= 8:
            return [wq.at[layer, :, pl.ds((idx - 8) * tile_heads, tile_heads), :]]
        if isinstance(idx, int) and idx >= 6:
            return [wkv.at[layer, :, idx - 6, :, :]]
        return [wqkv.at[layer, :, idx // 2, pl.ds(pl.multiple_of(lax.rem(idx, 2) * tile_heads, tile_heads), tile_heads), :]]

    def wo_src(layer):
        return [wo.at[layer, :, pl.ds(n * tile, tile)] for n in range(2)]

    def wc_src(layer):
        return [wc.at[layer, :, pl.ds(n * tile, tile)] for n in range(2)]

    def w1_src(layer, t):
        return [w1.at[layer, :, pl.ds((t * 3 + k) * tile, tile)] for k in range(3)]

    def w2_src(layer, t):
        return [w2.at[layer, pl.ds(k * depth, depth), pl.ds(t * tile, tile)] for k in range(3)]

    def project(dst, first, lhs, slot, wide):
        w = raw[slot].reshape(depth, tile)
        for n in range(tile // wide):
            put_blocks(dst, first + n * wide // LANES, dot(joined(lhs, range(blocks)), w[:, n * wide : (n + 1) * wide]).astype(BF16))

    def add_out(base):
        for k in range(2):
            for n in range(tile // piece):
                add_to_state(z, sums, (k * tile + n * piece) // LANES, dot(joined(xn, range(blocks)), ring_buf[base + k, :, n * piece : (n + 1) * piece]))

    load = block_copies(y_ref, first_row, z, io_sem)
    load_enc = block_copies(enc_ref, 0, enc, enc_sem)
    for copy in load:
        copy.start()
    raws.start(0, raw_src(0, 0))
    load_state(load, z, sums)
    settle_norm(sums, rstd, depth)
    raws.start(1, raw_src(0, 1))
    raws.start(2, raw_src(0, 2))
    ring.start(0, wo_src(0))

    for layer in range(layers):
        last = layer + 1 == layers
        shift = 10 * layer % 4
        bases = [((6 * layer + g) % 2) * 3 for g in range(7)]

        def raw_slot(idx):
            return (shift + idx) % 4

        def raw_ahead(idx):
            if idx + 3 < 10 or not last:
                raws.start(raw_slot(idx + 3), raw_src(layer, idx + 3))

        def qkv_step(j):
            slot = lax.rem(j + shift, 4)
            raws.wait(slot, raw_src(layer, 0))

            @pl.when(j < 3)
            def _():
                raws.start(lax.rem(j + shift + 3, 4), raw_src(layer, j + 3))

            for later in range(3, 6):

                @pl.when(j == later)
                def _(later=later):
                    raw_ahead(later)

            project(big, j * (tile // LANES), xn, slot, tile)

        normalize(z, rstd, xn)
        loop(6, qkv_step)

        if layer == 0:
            for copy in load_enc:
                copy.start()

        causal = lax.broadcasted_iota(jnp.int32, (span, span), 1) <= lax.broadcasted_iota(jnp.int32, (span, span), 0)

        def self_step(b):
            at = pl.ds(pl.multiple_of(b * span, span), span)

            def scores(u):
                return jnp.where(causal, dot_t(big[u, at], big[heads + u, at]), -1e30 / scale)

            def finish(u, probs):
                xn[u, at] = dot(probs, big[2 * heads + u, at]).astype(BF16)

            attend_units(heads, scores, scale, finish)

        loop(seqs, self_step)

        ring.wait(bases[0], wo_src(layer))
        ring.start(bases[1], wc_src(layer))
        add_out(bases[0])
        settle_norm(sums, rstd, depth)

        if layer == 0:
            for copy in load_enc:
                copy.wait()
        def kv_step(t):
            slot = lax.rem(t + shift + 6, 4)
            raws.wait(slot, raw_src(layer, 6))
            for later in range(2):

                @pl.when(t == later)
                def _(later=later):
                    raw_ahead(6 + later)

            project(kv, t * (tile // LANES), enc, slot, piece)

        loop(2, kv_step)

        def cross_q_step(t):
            slot = lax.rem(t + shift + 8, 4)
            raws.wait(slot, raw_src(layer, 8))
            for later in range(2):

                @pl.when(t == later)
                def _(later=later):
                    raw_ahead(8 + later)

            project(big, t * (tile // LANES), xn, slot, tile)

        normalize(z, rstd, xn)
        loop(2, cross_q_step)

        def cross_step(b):
            at = pl.ds(pl.multiple_of(b * span, span), span)
            at_kv = pl.ds(pl.multiple_of(b * ctx, ctx), ctx)
            keep = lax.broadcasted_iota(jnp.int32, (1, ctx), 1) < len_ref[b + first_len]

            def scores(g):
                query = jnp.concatenate([big[g * rep + r, at] for r in range(rep)], axis=0)
                return jnp.where(keep, dot_t(query, kv[g, at_kv]), -1e30 / scale)

            def finish(g, probs):
                mixed = dot(probs, kv[kv_heads + g, at_kv]).astype(BF16)
                for r in range(rep):
                    xn[g * rep + r, at] = mixed[r * span : (r + 1) * span]

            attend_units(kv_heads, scores, scale, finish)

        loop(seqs, cross_step)

        ring.wait(bases[1], wc_src(layer))
        ring.start(bases[2], w1_src(layer, 0))
        add_out(bases[1])
        settle_norm(sums, rstd, depth)

        def w1_step(t):
            base = jnp.where(t == 0, bases[2], bases[3])
            ring.wait(base, w1_src(layer, 0))

            @pl.when(t == 0)
            def _():
                ring.start(bases[3], w1_src(layer, 1))

            @pl.when(t == 1)
            def _():
                ring.start(bases[4], w2_src(layer, 0))

            ffn_in(xn, big, ring_buf, base, t, tile, piece, rows)

        normalize(z, rstd, xn)
        loop(2, w1_step)

        def w2_step(t):
            base = jnp.where(t == 0, bases[4], bases[5])
            ring.wait(base, w2_src(layer, 0))

            @pl.when(t == 0)
            def _():
                ring.start(bases[5], w2_src(layer, 1))

            if not last:

                @pl.when(t == 1)
                def _():
                    ring.start(bases[6], wo_src(layer + 1))

            ffn_out(z, sums, big, ring_buf, base, t, tile, piece)

        loop(2, w2_step)
        if not last:
            settle_norm(sums, rstd, depth)

    store = block_copies(out_ref, out_row, z, io_sem, to_hbm=True)
    for copy in store:
        copy.start()
    for copy in store:
        copy.wait()


def decoder_call(first_seq, seqs, y, first_len, enc_len, enc, out_seq, out_seqs, wqkv, wo, wq, wkv, wc, w1, w2):
    span, depth = y.shape[1], y.shape[2]
    layers, ff = wqkv.shape[0], w1.shape[2]
    heads = wqkv.shape[3]
    rows, tile, ctx = seqs * span, depth // 2, enc.shape[0]
    assert ff == 3 * depth and heads * HEAD == depth
    any_spec = pl.BlockSpec(memory_space=pl.ANY)
    per_layer = 2 * rows * depth * (6 * depth + 2 * ff) + 4 * ctx * depth * depth + 4 * seqs * heads * span * (span + ctx // seqs) * HEAD
    return pl.pallas_call(
        functools.partial(decoder_kernel, first_seq * span, out_seq * span, first_len, seqs, span),
        out_shape=jax.ShapeDtypeStruct((out_seqs * span, depth), BF16),
        in_specs=[pl.BlockSpec(memory_space=pltpu.SMEM)] + [any_spec] * 9,
        out_specs=any_spec,
        scratch_shapes=[
            pltpu.VMEM((depth // LANES, rows, LANES), BF16),
            pltpu.VMEM((depth // LANES, rows, LANES), BF16),
            pltpu.VMEM((ff // LANES, rows, LANES), BF16),
            pltpu.VMEM((depth // LANES, ctx, LANES), BF16),
            pltpu.VMEM((depth // LANES, ctx, LANES), BF16),
            pltpu.VMEM((rows, LANES), F32),
            pltpu.VMEM((rows, LANES), F32),
            pltpu.VMEM((4, depth, tile // HEAD, HEAD), BF16),
            pltpu.VMEM((6, depth, tile), BF16),
            pltpu.SemaphoreType.DMA((depth // LANES,)),
            pltpu.SemaphoreType.DMA((depth // LANES,)),
            pltpu.SemaphoreType.DMA((4,)),
            pltpu.SemaphoreType.DMA((6,)),
        ],
        compiler_params=pltpu.CompilerParams(vmem_limit_bytes=VMEM_LIMIT),
        cost_estimate=cost(layers * per_layer, 2 * layers * depth * (8 * depth + 2 * ff)),
        name="decode",
    )(
        enc_len,
        y.reshape(-1, depth),
        enc,
        wqkv,
        wo.reshape(layers, depth, depth),
        wq.reshape(layers, depth, heads, HEAD),
        wkv,
        wc.reshape(layers, depth, depth),
        w1,
        w2,
    )


def solution(mesh):
    stages = mesh.shape["stage"]
    swap = [(source, (source + stages // 2) % stages) for source in range(stages)]
    rows = P(("data", "stage"))
    whole = P()

    def body(x_enc, enc_len, y, enc_wqkv, enc_wo, enc_w1, enc_w2, dec_wqkv, dec_wo, cross_wq, cross_wkv, cross_wo, dec_w1, dec_w2):
        seqs, span, depth = y.shape
        half = seqs // 2
        enc_weights = (enc_wqkv, enc_wo, enc_w1, enc_w2)
        dec_weights = (dec_wqkv, dec_wo, cross_wq, cross_wkv, cross_wo, dec_w1, dec_w2)

        y_recv = lax.ppermute(y, "stage", swap)
        len_recv = lax.ppermute(enc_len, "stage", swap)
        home_enc = encoder_call(half, half, x_enc, enc_len, *enc_weights)
        home_recv = lax.ppermute(home_enc, "stage", swap)
        x_next, _ = lax.optimization_barrier((x_enc, home_enc))
        away_enc = encoder_call(0, half, x_next, enc_len, *enc_weights)
        away_out = decoder_call(0, half, y_recv, 0, enc_len, away_enc, 0, half, *dec_weights)
        out_recv = lax.ppermute(away_out, "stage", swap)
        y_next, _ = lax.optimization_barrier((y, away_out))
        home_out = decoder_call(half, half, y_next, half, len_recv, home_recv, half, seqs, *dec_weights)
        return lax.dynamic_update_slice(home_out, out_recv, (0, 0)).reshape(y.shape)

    return jax.shard_map(body, mesh=mesh, in_specs=(rows, rows, rows) + (whole,) * 11, out_specs=rows, check_vma=False)
```

```python
import functools

import jax
import jax.numpy as jnp
from jax import lax
from jax.experimental import pallas as pl
from jax.experimental.pallas import tpu as pltpu
from jax.sharding import PartitionSpec as P

HEAD = 128
LANES = 128
EPS = 1e-6
LOG2E = 1.4426950408889634
F32 = jnp.float32
BF16 = jnp.bfloat16
VMEM_LIMIT = 67043328


def dot(a, b):
    return jnp.dot(a, b, preferred_element_type=F32)


def dot_t(a, b):
    return lax.dot_general(a, b, (((1,), (1,)), ((), ())), preferred_element_type=F32)


def gelu(x):
    k = -2.0 * 0.7978845608028654 * LOG2E
    return x / (1.0 + jnp.exp2(x * (k + (k * 0.044715) * (x * x))))


def softmax_rows(scores, scale):
    top = jnp.max(scores, axis=-1, keepdims=True)
    weight = jnp.exp2((scores - top) * (scale * LOG2E))
    total = jnp.sum(weight, axis=-1, keepdims=True)
    return (weight * (1.0 / total)).astype(BF16)


def attend_units(count, make_scores, scale, finish, filler=()):
    done = 0
    ahead = make_scores(0)
    for i in range(count):
        now = ahead
        if i + 1 < count:
            ahead = make_scores(i + 1)
        upto = len(filler) * (i + 1) // count
        for piece in filler[done:upto]:
            piece()
        done = upto
        finish(i, softmax_rows(now, scale))


def joined(ref, blocks, rows=slice(None)):
    return jnp.concatenate([ref[c, rows] for c in blocks], axis=1)


def square_sum(ref, first, count):
    total = None
    for c in range(count):
        wide = ref[first + c].astype(F32)
        total = wide * wide if total is None else total + wide * wide
    return total


def settle_norm(sums, rstd, depth):
    mean = jnp.sum(sums[...], axis=-1, keepdims=True) * (1.0 / depth)
    rstd[...] = jnp.broadcast_to(lax.rsqrt(mean + EPS), rstd.shape)
    sums[...] = jnp.zeros_like(sums)


def normalize(state, rstd, dst):
    for c in range(state.shape[0]):
        dst[c] = (state[c].astype(F32) * rstd[...]).astype(BF16)


def add_to_state(state, sums, first, update, rows=slice(None)):
    part = None
    for k in range(update.shape[1] // LANES):
        fresh = (state[first + k, rows].astype(F32) + update[:, k * LANES : (k + 1) * LANES]).astype(BF16)
        state[first + k, rows] = fresh
        wide = fresh.astype(F32)
        part = wide * wide if part is None else part + wide * wide
    sums[rows] += part


def put_blocks(dst, first, value, rows=slice(None)):
    for k in range(value.shape[1] // LANES):
        dst[first + k, rows] = value[:, k * LANES : (k + 1) * LANES]


def block_copies(hbm, row0, buf, sems, to_hbm=False):
    blocks, rows = buf.shape[0], buf.shape[1]
    copies = []
    for c in range(blocks):
        there = hbm.at[pl.ds(row0, rows), pl.ds(c * LANES, LANES)]
        here = buf.at[c]
        copies.append(pltpu.make_async_copy(here, there, sems.at[c]) if to_hbm else pltpu.make_async_copy(there, here, sems.at[c]))
    return copies


class Ring:
    def __init__(self, buf, sem, split=False):
        self.buf, self.sem, self.split = buf, sem, split

    def start(self, base, refs):
        for k, ref in enumerate(refs):
            if self.split:
                for c in range(self.buf.shape[1]):
                    pltpu.make_async_copy(ref.at[:, pl.ds(c * LANES, LANES)], self.buf.at[base + k, c], self.sem.at[base + k]).start()
            else:
                pltpu.make_async_copy(ref, self.buf.at[base + k], self.sem.at[base + k]).start()

    def wait(self, base, refs):
        for k in range(len(refs)):
            slot = self.buf.at[base + k]
            pltpu.make_async_copy(slot, slot, self.sem.at[base + k]).wait()


def ring_cols(ring, slot, first, width):
    return jnp.concatenate([ring[slot, first // LANES + c] for c in range(width // LANES)], axis=1)


def at_cols(i, width):
    return pl.ds(pl.multiple_of(i * width, width), width)


def loop(count, step):
    def body(i, carry):
        step(i)
        return carry

    lax.fori_loop(0, count, body, 0)


def load_state(copies, state, sums):
    for c, copy in enumerate(copies):
        copy.wait()
        part = square_sum(state, c, 1)
        if c == 0:
            sums[...] = part
        else:
            sums[...] += part


def ffn_in(xn, big, ring, base, t, tile, piece, row_piece):
    blocks = range(xn.shape[0])
    for k in range(3):
        for n in range(tile // piece):
            w = ring_cols(ring, base + k, n * piece, piece)
            for m in range(xn.shape[1] // row_piece):
                rows = slice(m * row_piece, (m + 1) * row_piece)
                put_blocks(big, t * (3 * tile // LANES) + (k * tile + n * piece) // LANES, gelu(dot(joined(xn, blocks, rows), w)).astype(BF16), rows)


def ffn_out(state, sums, big, ring, base, t, tile, piece):
    depth_blocks = state.shape[0]
    for n in range(tile // piece):
        total = None
        for k in range(3):
            part = dot(joined(big, range(k * depth_blocks, (k + 1) * depth_blocks)), ring_cols(ring, base + k, n * piece, piece))
            total = part if total is None else total + part
        add_to_state(state, sums, t * (tile // LANES) + n * piece // LANES, total)


def cost(flops, bytes_accessed):
    return pl.CostEstimate(flops=int(flops), bytes_accessed=int(bytes_accessed), transcendentals=0)


def encoder_kernel(first_row, seqs, span, len_ref, x_ref, wqkv, wo, w1, w2, out_ref, h, xn, big, sums, rstd, raw, ring_buf, io_sem, raw_sem, ring_sem):
    layers, depth = wqkv.shape[0], wqkv.shape[1]
    heads = wqkv.shape[3]
    rows = seqs * span
    tile = depth // 2
    tile_heads = tile // HEAD
    piece = min(512, tile)
    row_piece = min(256, rows)
    blocks = depth // LANES
    n_qkv = 6
    scale = HEAD**-0.5

    raws = Ring(raw, raw_sem)
    ring = Ring(ring_buf, ring_sem, split=True)

    def qkv_src(layer, j):
        return [wqkv.at[layer, :, j // 2, pl.ds(pl.multiple_of(lax.rem(j, 2) * tile_heads, tile_heads), tile_heads), :]]

    def wo_src(layer):
        return [wo.at[layer, :, pl.ds(n * tile, tile)] for n in range(2)]

    def w1_src(layer, t):
        return [w1.at[layer, :, pl.ds((t * 3 + k) * tile, tile)] for k in range(3)]

    def w2_src(layer, t):
        return [w2.at[layer, pl.ds(k * depth, depth), pl.ds(t * tile, tile)] for k in range(3)]

    load = block_copies(x_ref, first_row, h, io_sem)
    for copy in load:
        copy.start()
    raws.start(0, qkv_src(0, 0))
    load_state(load, h, sums)
    settle_norm(sums, rstd, depth)
    ring.start(0, wo_src(0))

    for layer in range(layers):
        last = layer + 1 == layers
        bases = [((5 * layer + g) % 2) * 3 for g in range(6)]

        def qkv_step(j):
            slot = lax.rem(j, 2)
            raws.wait(slot, qkv_src(layer, j))

            @pl.when(j < n_qkv - 1)
            def _():
                raws.start(1 - slot, qkv_src(layer, j + 1))

            if not last:

                @pl.when(j == n_qkv - 1)
                def _():
                    raws.start(0, qkv_src(layer + 1, 0))

            normalize(h, rstd, xn)
            w = raw[slot].reshape(depth, tile)
            for n in range(tile // piece):
                put_blocks(big, j * (tile // LANES) + n * piece // LANES, dot(joined(xn, range(blocks)), w[:, n * piece : (n + 1) * piece]).astype(BF16))

        loop(n_qkv, qkv_step)

        def attention(b, at, first_head, count, filler=()):
            keep = lax.broadcasted_iota(jnp.int32, (1, span), 1) < len_ref[b + first_row // span]

            def scores(u):
                return jnp.where(keep, dot_t(big[first_head + u, at], big[heads + first_head + u, at]), -1e30 / scale)

            def finish(u, probs):
                xn[first_head + u, at] = dot(probs, big[2 * heads + first_head + u, at]).astype(BF16)

            attend_units(count, scores, scale, finish, filler)

        def attend_step(i):
            groups = heads // tile_heads
            b, g = i // groups, lax.rem(i, groups)
            attention(b, pl.ds(pl.multiple_of(b * span, span), span), g * tile_heads, tile_heads)

        loop((seqs - 1) * (heads // tile_heads), attend_step)

        def out_piece(n, at):
            w = ring_cols(ring_buf, bases[0] + n * piece // tile, (n * piece) % tile, piece)
            add_to_state(h, sums, n * piece // LANES, dot(joined(xn, range(blocks), at), w), at)

        ring.wait(bases[0], wo_src(layer))
        ring.start(bases[1], w1_src(layer, 0))
        n_out = depth // piece
        before = [slice(b * span, (b + 1) * span) for b in range(seqs - 1)]
        final = slice((seqs - 1) * span, seqs * span)
        attention(seqs - 1, final, 0, heads, [functools.partial(out_piece, n, at) for at in before for n in range(n_out)])
        for n in range(n_out):
            out_piece(n, final)
        settle_norm(sums, rstd, depth)

        def w1_step(t):
            base = jnp.where(t == 0, bases[1], bases[2])
            ring.wait(base, w1_src(layer, 0))

            @pl.when(t == 0)
            def _():
                ring.start(bases[2], w1_src(layer, 1))

            @pl.when(t == 1)
            def _():
                ring.start(bases[3], w2_src(layer, 0))

            normalize(h, rstd, xn)
            ffn_in(xn, big, ring_buf, base, t, tile, piece, row_piece)

        loop(2, w1_step)

        def w2_step(t):
            base = jnp.where(t == 0, bases[3], bases[4])
            ring.wait(base, w2_src(layer, 0))

            @pl.when(t == 0)
            def _():
                ring.start(bases[4], w2_src(layer, 1))

            if not last:

                @pl.when(t == 1)
                def _():
                    ring.start(bases[5], wo_src(layer + 1))

            ffn_out(h, sums, big, ring_buf, base, t, tile, piece)

        loop(2, w2_step)
        settle_norm(sums, rstd, depth)

    normalize(h, rstd, xn)
    store = block_copies(out_ref, 0, xn, io_sem, to_hbm=True)
    for copy in store:
        copy.start()
    for copy in store:
        copy.wait()


def encoder_call(first_seq, seqs, x, enc_len, wqkv, wo, w1, w2):
    span, depth = x.shape[1], x.shape[2]
    layers, ff = wqkv.shape[0], w1.shape[2]
    rows, tile = seqs * span, depth // 2
    heads = wqkv.shape[3]
    assert ff == 3 * depth and heads * HEAD == depth
    any_spec = pl.BlockSpec(memory_space=pl.ANY)
    per_layer = 2 * rows * depth * (4 * depth + 2 * ff) + 4 * seqs * heads * span * span * HEAD
    return pl.pallas_call(
        functools.partial(encoder_kernel, first_seq * span, seqs, span),
        out_shape=jax.ShapeDtypeStruct((rows, depth), BF16),
        in_specs=[pl.BlockSpec(memory_space=pltpu.SMEM)] + [any_spec] * 5,
        out_specs=any_spec,
        scratch_shapes=[
            pltpu.VMEM((depth // LANES, rows, LANES), BF16),
            pltpu.VMEM((depth // LANES, rows, LANES), BF16),
            pltpu.VMEM((ff // LANES, rows, LANES), BF16),
            pltpu.VMEM((rows, LANES), F32),
            pltpu.VMEM((rows, LANES), F32),
            pltpu.VMEM((2, depth, tile // HEAD, HEAD), BF16),
            pltpu.VMEM((6, tile // LANES, depth, LANES), BF16),
            pltpu.SemaphoreType.DMA((depth // LANES,)),
            pltpu.SemaphoreType.DMA((2,)),
            pltpu.SemaphoreType.DMA((6,)),
        ],
        compiler_params=pltpu.CompilerParams(vmem_limit_bytes=VMEM_LIMIT),
        cost_estimate=cost(layers * per_layer, 2 * layers * depth * (4 * depth + 2 * ff)),
        name="encode",
    )(enc_len, x.reshape(-1, depth), wqkv, wo.reshape(layers, depth, depth), w1, w2)


def decoder_kernel(first_row, out_row, first_len, seqs, span, len_ref, y_ref, enc_ref, wqkv, wo, wq, wkv, wc, w1, w2, out_ref, z, xn, big, enc, kv, sums, rstd, raw, ring_buf, io_sem, enc_sem, raw_sem, ring_sem):
    layers, depth = wqkv.shape[0], wqkv.shape[1]
    heads = wqkv.shape[3]
    kv_heads = wkv.shape[3]
    rep = heads // kv_heads
    rows = z.shape[1]
    ctx = enc.shape[1] // seqs
    tile = depth // 2
    tile_heads = tile // HEAD
    piece = min(512, tile)
    blocks = depth // LANES
    scale = HEAD**-0.5

    raws = Ring(raw, raw_sem)
    ring = Ring(ring_buf, ring_sem, split=True)

    def raw_src(layer, idx):
        if isinstance(idx, int) and idx >= 10:
            return raw_src(layer + 1, idx - 10)
        if isinstance(idx, int) and idx >= 8:
            return [wq.at[layer, :, pl.ds((idx - 8) * tile_heads, tile_heads), :]]
        if isinstance(idx, int) and idx >= 6:
            return [wkv.at[layer, :, idx - 6, :, :]]
        return [wqkv.at[layer, :, idx // 2, pl.ds(pl.multiple_of(lax.rem(idx, 2) * tile_heads, tile_heads), tile_heads), :]]

    def wo_src(layer):
        return [wo.at[layer, :, pl.ds(n * tile, tile)] for n in range(2)]

    def wc_src(layer):
        return [wc.at[layer, :, pl.ds(n * tile, tile)] for n in range(2)]

    def w1_src(layer, t):
        return [w1.at[layer, :, pl.ds((t * 3 + k) * tile, tile)] for k in range(3)]

    def w2_src(layer, t):
        return [w2.at[layer, pl.ds(k * depth, depth), pl.ds(t * tile, tile)] for k in range(3)]

    def project(dst, first, lhs, slot, wide):
        w = raw[slot].reshape(depth, tile)
        for n in range(tile // wide):
            put_blocks(dst, first + n * wide // LANES, dot(joined(lhs, range(blocks)), w[:, n * wide : (n + 1) * wide]).astype(BF16))

    def out_piece(base, n, at):
        w = ring_cols(ring_buf, base + n * piece // tile, (n * piece) % tile, piece)
        add_to_state(z, sums, n * piece // LANES, dot(joined(xn, range(blocks), at), w), at)

    n_out = depth // piece
    every = slice(0, rows)
    before = [slice(b * span, (b + 1) * span) for b in range(seqs - 1)]
    final = slice((seqs - 1) * span, seqs * span)

    load = block_copies(y_ref, first_row, z, io_sem)
    load_enc = block_copies(enc_ref, 0, enc, enc_sem)
    for copy in load:
        copy.start()
    raws.start(0, raw_src(0, 0))
    load_state(load, z, sums)
    settle_norm(sums, rstd, depth)
    raws.start(1, raw_src(0, 1))
    ring.start(0, wo_src(0))

    for layer in range(layers):
        last = layer + 1 == layers
        shift = 10 * layer % 3
        bases = [((6 * layer + g) % 2) * 3 for g in range(7)]

        def raw_slot(idx):
            return (shift + idx) % 3

        def raw_ahead(idx):
            if idx + 2 < 10 or not last:
                raws.start(raw_slot(idx + 2), raw_src(layer, idx + 2))

        def qkv_step(j):
            slot = lax.rem(j + shift, 3)
            raws.wait(slot, raw_src(layer, 0))

            @pl.when(j < 4)
            def _():
                raws.start(lax.rem(j + shift + 2, 3), raw_src(layer, j + 2))

            for later in range(4, 6):

                @pl.when(j == later)
                def _(later=later):
                    raw_ahead(later)

            project(big, j * (tile // LANES), xn, slot, tile)

        normalize(z, rstd, xn)
        if layer == 0:
            for copy in load_enc:
                copy.start()
        loop(6, qkv_step)

        if layer == 0:
            for copy in load_enc:
                copy.wait()

        causal = lax.broadcasted_iota(jnp.int32, (span, span), 1) <= lax.broadcasted_iota(jnp.int32, (span, span), 0)

        def self_step(b):
            slot = lax.rem(b + shift + 6, 3)
            raws.wait(slot, raw_src(layer, 6))
            for later in range(2):

                @pl.when(b == later)
                def _(later=later):
                    raw_ahead(6 + later)

            at = pl.ds(pl.multiple_of(b * span, span), span)
            w = raw[slot].reshape(depth, tile)
            kv_rows = min(256, kv.shape[1])

            def kv_piece(n, m):
                part = slice(m * kv_rows, (m + 1) * kv_rows)
                put_blocks(kv, b * (tile // LANES) + n * piece // LANES, dot(joined(enc, range(blocks), part), w[:, n * piece : (n + 1) * piece]).astype(BF16), part)

            def scores(u):
                return jnp.where(causal, dot_t(big[u, at], big[heads + u, at]), -1e30 / scale)

            def finish(u, probs):
                xn[u, at] = dot(probs, big[2 * heads + u, at]).astype(BF16)

            pieces = [functools.partial(kv_piece, n, m) for n in range(tile // piece) for m in range(kv.shape[1] // kv_rows)]
            attend_units(heads, scores, scale, finish, pieces)

        loop(2, self_step)

        ring.wait(bases[0], wo_src(layer))
        ring.start(bases[1], wc_src(layer))
        for n in range(n_out):
            out_piece(bases[0], n, every)
        settle_norm(sums, rstd, depth)

        def cross_q_step(t):
            slot = lax.rem(t + shift + 8, 3)
            raws.wait(slot, raw_src(layer, 8))
            for later in range(2):

                @pl.when(t == later)
                def _(later=later):
                    raw_ahead(8 + later)

            project(big, t * (tile // LANES), xn, slot, tile)

        normalize(z, rstd, xn)
        loop(2, cross_q_step)

        def cross(b, at, at_kv, filler=()):
            keep = lax.broadcasted_iota(jnp.int32, (1, ctx), 1) < len_ref[b + first_len]

            def scores(g):
                query = jnp.concatenate([big[g * rep + r, at] for r in range(rep)], axis=0)
                return jnp.where(keep, dot_t(query, kv[g, at_kv]), -1e30 / scale)

            def finish(g, probs):
                mixed = dot(probs, kv[kv_heads + g, at_kv]).astype(BF16)
                for r in range(rep):
                    xn[g * rep + r, at] = mixed[r * span : (r + 1) * span]

            attend_units(kv_heads, scores, scale, finish, filler)

        ring.wait(bases[1], wc_src(layer))
        ring.start(bases[2], w1_src(layer, 0))
        for b in range(seqs - 1):
            cross(b, before[b], slice(b * ctx, (b + 1) * ctx))
        pieces = [functools.partial(out_piece, bases[1], n, at) for at in before for n in range(n_out)]
        cross(seqs - 1, final, slice((seqs - 1) * ctx, seqs * ctx), pieces)
        for n in range(n_out):
            out_piece(bases[1], n, final)
        settle_norm(sums, rstd, depth)

        def w1_step(t):
            base = jnp.where(t == 0, bases[2], bases[3])
            ring.wait(base, w1_src(layer, 0))

            @pl.when(t == 0)
            def _():
                ring.start(bases[3], w1_src(layer, 1))

            @pl.when(t == 1)
            def _():
                ring.start(bases[4], w2_src(layer, 0))

            ffn_in(xn, big, ring_buf, base, t, tile, tile, rows // 2)

        normalize(z, rstd, xn)
        loop(2, w1_step)

        def w2_step(t):
            base = jnp.where(t == 0, bases[4], bases[5])
            ring.wait(base, w2_src(layer, 0))

            @pl.when(t == 0)
            def _():
                ring.start(bases[5], w2_src(layer, 1))

            if not last:

                @pl.when(t == 1)
                def _():
                    ring.start(bases[6], wo_src(layer + 1))

            ffn_out(z, sums, big, ring_buf, base, t, tile, piece)

        loop(2, w2_step)
        if not last:
            settle_norm(sums, rstd, depth)

    store = block_copies(out_ref, out_row, z, io_sem, to_hbm=True)
    for copy in store:
        copy.start()
    for copy in store:
        copy.wait()


def decoder_call(first_seq, seqs, y, first_len, enc_len, enc, out_seq, out_seqs, wqkv, wo, wq, wkv, wc, w1, w2):
    span, depth = y.shape[1], y.shape[2]
    layers, ff = wqkv.shape[0], w1.shape[2]
    heads = wqkv.shape[3]
    rows, tile, ctx = seqs * span, depth // 2, enc.shape[0]
    assert ff == 3 * depth and heads * HEAD == depth and seqs == 2
    any_spec = pl.BlockSpec(memory_space=pl.ANY)
    per_layer = 2 * rows * depth * (6 * depth + 2 * ff) + 4 * ctx * depth * depth + 4 * seqs * heads * span * (span + ctx // seqs) * HEAD
    return pl.pallas_call(
        functools.partial(decoder_kernel, first_seq * span, out_seq * span, first_len, seqs, span),
        out_shape=jax.ShapeDtypeStruct((out_seqs * span, depth), BF16),
        in_specs=[pl.BlockSpec(memory_space=pltpu.SMEM)] + [any_spec] * 9,
        out_specs=any_spec,
        scratch_shapes=[
            pltpu.VMEM((depth // LANES, rows, LANES), BF16),
            pltpu.VMEM((depth // LANES, rows, LANES), BF16),
            pltpu.VMEM((ff // LANES, rows, LANES), BF16),
            pltpu.VMEM((depth // LANES, ctx, LANES), BF16),
            pltpu.VMEM((depth // LANES, ctx, LANES), BF16),
            pltpu.VMEM((rows, LANES), F32),
            pltpu.VMEM((rows, LANES), F32),
            pltpu.VMEM((3, depth, tile // HEAD, HEAD), BF16),
            pltpu.VMEM((6, tile // LANES, depth, LANES), BF16),
            pltpu.SemaphoreType.DMA((depth // LANES,)),
            pltpu.SemaphoreType.DMA((depth // LANES,)),
            pltpu.SemaphoreType.DMA((3,)),
            pltpu.SemaphoreType.DMA((6,)),
        ],
        compiler_params=pltpu.CompilerParams(vmem_limit_bytes=VMEM_LIMIT),
        cost_estimate=cost(layers * per_layer, 2 * layers * depth * (8 * depth + 2 * ff)),
        name="decode",
    )(
        enc_len,
        y.reshape(-1, depth),
        enc,
        wqkv,
        wo.reshape(layers, depth, depth),
        wq.reshape(layers, depth, heads, HEAD),
        wkv,
        wc.reshape(layers, depth, depth),
        w1,
        w2,
    )


def solution(mesh):
    stages = mesh.shape["stage"]
    swap = [(source, (source + stages // 2) % stages) for source in range(stages)]
    rows = P(("data", "stage"))
    whole = P()

    def body(x_enc, enc_len, y, enc_wqkv, enc_wo, enc_w1, enc_w2, dec_wqkv, dec_wo, cross_wq, cross_wkv, cross_wo, dec_w1, dec_w2):
        seqs, span, depth = y.shape
        half = seqs // 2
        enc_weights = (enc_wqkv, enc_wo, enc_w1, enc_w2)
        dec_weights = (dec_wqkv, dec_wo, cross_wq, cross_wkv, cross_wo, dec_w1, dec_w2)

        y_recv = lax.ppermute(y, "stage", swap)
        len_recv = lax.ppermute(enc_len, "stage", swap)
        home_enc = encoder_call(half, half, x_enc, enc_len, *enc_weights)
        home_recv = lax.ppermute(home_enc, "stage", swap)
        x_next, _ = lax.optimization_barrier((x_enc, home_enc))
        away_enc = encoder_call(0, half, x_next, enc_len, *enc_weights)
        away_out = decoder_call(0, half, y_recv, 0, enc_len, away_enc, 0, half, *dec_weights)
        out_recv = lax.ppermute(away_out, "stage", swap)
        y_next, _ = lax.optimization_barrier((y, away_out))
        home_out = decoder_call(half, half, y_next, half, len_recv, home_recv, half, seqs, *dec_weights)
        return lax.dynamic_update_slice(home_out, out_recv, (0, 0)).reshape(y.shape)

    return jax.shard_map(body, mesh=mesh, in_specs=(rows, rows, rows) + (whole,) * 11, out_specs=rows, check_vma=False)
```

```python
import functools

import jax
import jax.numpy as jnp
from jax import lax
from jax.experimental import pallas as pl
from jax.experimental.pallas import tpu as pltpu
from jax.sharding import PartitionSpec as P

HEAD = 128
LANES = 128
EPS = 1e-6
LOG2E = 1.4426950408889634
F32 = jnp.float32
BF16 = jnp.bfloat16
VMEM_LIMIT = 67043328


def dot(a, b):
    return jnp.dot(a, b, preferred_element_type=F32)


def dot_t(a, b):
    return lax.dot_general(a, b, (((1,), (1,)), ((), ())), preferred_element_type=F32)


def gelu(x):
    k = -2.0 * 0.7978845608028654 * LOG2E
    return x / (1.0 + jnp.exp2(x * (k + (k * 0.044715) * (x * x))))


def softmax_rows(scores, scale):
    top = jnp.max(scores, axis=-1, keepdims=True)
    weight = jnp.exp2((scores - top) * (scale * LOG2E))
    total = jnp.sum(weight, axis=-1, keepdims=True)
    return (weight * (1.0 / total)).astype(BF16)


def attend_units(count, make_scores, scale, finish, filler=()):
    done = 0
    ahead = make_scores(0)
    for i in range(count):
        now = ahead
        if i + 1 < count:
            ahead = make_scores(i + 1)
        upto = len(filler) * (i + 1) // count
        for piece in filler[done:upto]:
            piece()
        done = upto
        finish(i, softmax_rows(now, scale))


def joined(ref, blocks, rows=slice(None)):
    return jnp.concatenate([ref[c, rows] for c in blocks], axis=1)


def square_sum(ref, first, count):
    total = None
    for c in range(count):
        wide = ref[first + c].astype(F32)
        total = wide * wide if total is None else total + wide * wide
    return total


def settle_norm(sums, rstd, depth):
    mean = jnp.sum(sums[...], axis=-1, keepdims=True) * (1.0 / depth)
    rstd[...] = jnp.broadcast_to(lax.rsqrt(mean + EPS), rstd.shape)
    sums[...] = jnp.zeros_like(sums)


def normalize(state, rstd, dst):
    for c in range(state.shape[0]):
        dst[c] = (state[c].astype(F32) * rstd[...]).astype(BF16)


def add_to_state(state, sums, first, update, rows=slice(None)):
    part = None
    for k in range(update.shape[1] // LANES):
        fresh = (state[first + k, rows].astype(F32) + update[:, k * LANES : (k + 1) * LANES]).astype(BF16)
        state[first + k, rows] = fresh
        wide = fresh.astype(F32)
        part = wide * wide if part is None else part + wide * wide
    sums[rows] += part


def put_blocks(dst, first, value, rows=slice(None)):
    for k in range(value.shape[1] // LANES):
        dst[first + k, rows] = value[:, k * LANES : (k + 1) * LANES]


def block_copies(hbm, row0, buf, sems, to_hbm=False):
    blocks, rows = buf.shape[0], buf.shape[1]
    copies = []
    for c in range(blocks):
        there = hbm.at[pl.ds(row0, rows), pl.ds(c * LANES, LANES)]
        here = buf.at[c]
        copies.append(pltpu.make_async_copy(here, there, sems.at[c]) if to_hbm else pltpu.make_async_copy(there, here, sems.at[c]))
    return copies


class Ring:
    def __init__(self, buf, sem, split=False):
        self.buf, self.sem, self.split = buf, sem, split

    def start(self, base, refs):
        for k, ref in enumerate(refs):
            if self.split:
                for c in range(self.buf.shape[1]):
                    pltpu.make_async_copy(ref.at[:, pl.ds(c * LANES, LANES)], self.buf.at[base + k, c], self.sem.at[base + k]).start()
            else:
                pltpu.make_async_copy(ref, self.buf.at[base + k], self.sem.at[base + k]).start()

    def wait(self, base, refs):
        for k in range(len(refs)):
            slot = self.buf.at[base + k]
            pltpu.make_async_copy(slot, slot, self.sem.at[base + k]).wait()


def ring_cols(ring, slot, first, width):
    return jnp.concatenate([ring[slot, first // LANES + c] for c in range(width // LANES)], axis=1)


def at_cols(i, width):
    return pl.ds(pl.multiple_of(i * width, width), width)


def loop(count, step):
    def body(i, carry):
        step(i)
        return carry

    lax.fori_loop(0, count, body, 0)


def load_state(copies, state, sums):
    for c, copy in enumerate(copies):
        copy.wait()
        part = square_sum(state, c, 1)
        if c == 0:
            sums[...] = part
        else:
            sums[...] += part


def ffn_in(xn, big, ring, base, t, tile, piece, row_piece):
    blocks = range(xn.shape[0])
    for k in range(3):
        for n in range(tile // piece):
            w = ring_cols(ring, base + k, n * piece, piece)
            for m in range(xn.shape[1] // row_piece):
                rows = slice(m * row_piece, (m + 1) * row_piece)
                put_blocks(big, t * (3 * tile // LANES) + (k * tile + n * piece) // LANES, gelu(dot(joined(xn, blocks, rows), w)).astype(BF16), rows)


def ffn_out(state, sums, big, ring, base, t, tile, piece):
    depth_blocks = state.shape[0]
    for n in range(tile // piece):
        total = None
        for k in range(3):
            part = dot(joined(big, range(k * depth_blocks, (k + 1) * depth_blocks)), ring_cols(ring, base + k, n * piece, piece))
            total = part if total is None else total + part
        add_to_state(state, sums, t * (tile // LANES) + n * piece // LANES, total)


def cost(flops, bytes_accessed):
    return pl.CostEstimate(flops=int(flops), bytes_accessed=int(bytes_accessed), transcendentals=0)


def encoder_kernel(first_row, seqs, span, len_ref, x_ref, wqkv, wo, w1, w2, out_ref, h, xn, big, sums, rstd, raw, ring_buf, io_sem, raw_sem, ring_sem):
    layers, depth = wqkv.shape[0], wqkv.shape[1]
    heads = wqkv.shape[3]
    rows = seqs * span
    tile = depth // 2
    tile_heads = tile // HEAD
    piece = min(512, tile)
    row_piece = min(256, rows)
    blocks = depth // LANES
    n_qkv = 6
    scale = HEAD**-0.5

    raws = Ring(raw, raw_sem)
    ring = Ring(ring_buf, ring_sem, split=True)

    def qkv_src(layer, j):
        return [wqkv.at[layer, :, j // 2, pl.ds(pl.multiple_of(lax.rem(j, 2) * tile_heads, tile_heads), tile_heads), :]]

    def wo_src(layer):
        return [wo.at[layer, :, pl.ds(n * tile, tile)] for n in range(2)]

    def w1_src(layer, t):
        return [w1.at[layer, :, pl.ds((t * 3 + k) * tile, tile)] for k in range(3)]

    def w2_src(layer, t):
        return [w2.at[layer, pl.ds(k * depth, depth), pl.ds(t * tile, tile)] for k in range(3)]

    load = block_copies(x_ref, first_row, h, io_sem)
    for copy in load:
        copy.start()
    raws.start(0, qkv_src(0, 0))
    load_state(load, h, sums)
    settle_norm(sums, rstd, depth)

    for layer in range(layers):
        last = layer + 1 == layers
        bases = [((5 * layer + g) % 2) * 3 for g in range(6)]

        def qkv_step(j):
            slot = lax.rem(j, 2)
            raws.wait(slot, qkv_src(layer, j))

            @pl.when(j < n_qkv - 1)
            def _():
                raws.start(1 - slot, qkv_src(layer, j + 1))

            if not last:

                @pl.when(j == n_qkv - 1)
                def _():
                    raws.start(0, qkv_src(layer + 1, 0))

            normalize(h, rstd, xn)
            w = raw[slot].reshape(depth, tile)
            for n in range(tile // piece):
                put_blocks(big, j * (tile // LANES) + n * piece // LANES, dot(joined(xn, range(blocks)), w[:, n * piece : (n + 1) * piece]).astype(BF16))

        loop(n_qkv, qkv_step)
        if layer == 0:
            ring.start(bases[0], wo_src(0))

        def attention(b, at, first_head, count, filler=()):
            keep = lax.broadcasted_iota(jnp.int32, (1, span), 1) < len_ref[b + first_row // span]

            def scores(u):
                return jnp.where(keep, dot_t(big[first_head + u, at], big[heads + first_head + u, at]), -1e30 / scale)

            def finish(u, probs):
                xn[first_head + u, at] = dot(probs, big[2 * heads + first_head + u, at]).astype(BF16)

            attend_units(count, scores, scale, finish, filler)

        def attend_step(i):
            groups = heads // tile_heads
            b, g = i // groups, lax.rem(i, groups)
            attention(b, pl.ds(pl.multiple_of(b * span, span), span), g * tile_heads, tile_heads)

        loop((seqs - 1) * (heads // tile_heads), attend_step)

        def out_piece(n, at):
            w = ring_cols(ring_buf, bases[0] + n * piece // tile, (n * piece) % tile, piece)
            add_to_state(h, sums, n * piece // LANES, dot(joined(xn, range(blocks), at), w), at)

        ring.wait(bases[0], wo_src(layer))
        ring.start(bases[1], w1_src(layer, 0))
        n_out = depth // piece
        half_span = span // 2
        before = [slice(b * half_span, (b + 1) * half_span) for b in range(2 * (seqs - 1))]
        final = slice((seqs - 1) * span, seqs * span)
        attention(seqs - 1, final, 0, heads, [functools.partial(out_piece, n, at) for at in before for n in range(n_out)])
        for n in range(n_out):
            out_piece(n, final)
        settle_norm(sums, rstd, depth)

        def w1_step(t):
            base = jnp.where(t == 0, bases[1], bases[2])
            ring.wait(base, w1_src(layer, 0))

            @pl.when(t == 0)
            def _():
                ring.start(bases[2], w1_src(layer, 1))

            @pl.when(t == 1)
            def _():
                ring.start(bases[3], w2_src(layer, 0))

            normalize(h, rstd, xn)
            ffn_in(xn, big, ring_buf, base, t, tile, piece, row_piece)

        loop(2, w1_step)

        def w2_step(t):
            base = jnp.where(t == 0, bases[3], bases[4])
            ring.wait(base, w2_src(layer, 0))

            @pl.when(t == 0)
            def _():
                ring.start(bases[4], w2_src(layer, 1))

            if not last:

                @pl.when(t == 1)
                def _():
                    ring.start(bases[5], wo_src(layer + 1))

            ffn_out(h, sums, big, ring_buf, base, t, tile, piece)

        loop(2, w2_step)
        settle_norm(sums, rstd, depth)

    normalize(h, rstd, xn)
    store = block_copies(out_ref, 0, xn, io_sem, to_hbm=True)
    for copy in store:
        copy.start()
    for copy in store:
        copy.wait()


def encoder_call(first_seq, seqs, x, enc_len, wqkv, wo, w1, w2):
    span, depth = x.shape[1], x.shape[2]
    layers, ff = wqkv.shape[0], w1.shape[2]
    rows, tile = seqs * span, depth // 2
    heads = wqkv.shape[3]
    assert ff == 3 * depth and heads * HEAD == depth
    any_spec = pl.BlockSpec(memory_space=pl.ANY)
    per_layer = 2 * rows * depth * (4 * depth + 2 * ff) + 4 * seqs * heads * span * span * HEAD
    return pl.pallas_call(
        functools.partial(encoder_kernel, first_seq * span, seqs, span),
        out_shape=jax.ShapeDtypeStruct((rows, depth), BF16),
        in_specs=[pl.BlockSpec(memory_space=pltpu.SMEM)] + [any_spec] * 5,
        out_specs=any_spec,
        scratch_shapes=[
            pltpu.VMEM((depth // LANES, rows, LANES), BF16),
            pltpu.VMEM((depth // LANES, rows, LANES), BF16),
            pltpu.VMEM((ff // LANES, rows, LANES), BF16),
            pltpu.VMEM((rows, LANES), F32),
            pltpu.VMEM((rows, LANES), F32),
            pltpu.VMEM((2, depth, tile // HEAD, HEAD), BF16),
            pltpu.VMEM((6, tile // LANES, depth, LANES), BF16),
            pltpu.SemaphoreType.DMA((depth // LANES,)),
            pltpu.SemaphoreType.DMA((2,)),
            pltpu.SemaphoreType.DMA((6,)),
        ],
        compiler_params=pltpu.CompilerParams(vmem_limit_bytes=VMEM_LIMIT),
        cost_estimate=cost(layers * per_layer, 2 * layers * depth * (4 * depth + 2 * ff)),
        name="encode",
    )(enc_len, x.reshape(-1, depth), wqkv, wo.reshape(layers, depth, depth), w1, w2)


def decoder_kernel(first_row, out_row, first_len, seqs, span, len_ref, y_ref, enc_ref, wqkv, wo, wq, wkv, wc, w1, w2, out_ref, z, xn, big, enc, kv, sums, rstd, raw, ring_buf, io_sem, enc_sem, raw_sem, ring_sem):
    layers, depth = wqkv.shape[0], wqkv.shape[1]
    heads = wqkv.shape[3]
    kv_heads = wkv.shape[3]
    rep = heads // kv_heads
    rows = z.shape[1]
    ctx = enc.shape[1] // seqs
    tile = depth // 2
    tile_heads = tile // HEAD
    piece = min(512, tile)
    blocks = depth // LANES
    scale = HEAD**-0.5

    raws = Ring(raw, raw_sem)
    ring = Ring(ring_buf, ring_sem, split=True)

    def raw_src(layer, idx):
        if isinstance(idx, int) and idx >= 10:
            return raw_src(layer + 1, idx - 10)
        if isinstance(idx, int) and idx >= 8:
            return [wq.at[layer, :, pl.ds((idx - 8) * tile_heads, tile_heads), :]]
        if isinstance(idx, int) and idx >= 6:
            return [wkv.at[layer, :, idx - 6, :, :]]
        return [wqkv.at[layer, :, idx // 2, pl.ds(pl.multiple_of(lax.rem(idx, 2) * tile_heads, tile_heads), tile_heads), :]]

    def wo_src(layer):
        return [wo.at[layer, :, pl.ds(n * tile, tile)] for n in range(2)]

    def wc_src(layer):
        return [wc.at[layer, :, pl.ds(n * tile, tile)] for n in range(2)]

    def w1_src(layer, t):
        return [w1.at[layer, :, pl.ds((t * 3 + k) * tile, tile)] for k in range(3)]

    def w2_src(layer, t):
        return [w2.at[layer, pl.ds(k * depth, depth), pl.ds(t * tile, tile)] for k in range(3)]

    def project(dst, first, lhs, slot, wide):
        w = raw[slot].reshape(depth, tile)
        for n in range(tile // wide):
            put_blocks(dst, first + n * wide // LANES, dot(joined(lhs, range(blocks)), w[:, n * wide : (n + 1) * wide]).astype(BF16))

    def out_piece(base, n, at):
        w = ring_cols(ring_buf, base + n * piece // tile, (n * piece) % tile, piece)
        add_to_state(z, sums, n * piece // LANES, dot(joined(xn, range(blocks), at), w), at)

    n_out = depth // piece
    every = slice(0, rows)
    before = [slice(b * span, (b + 1) * span) for b in range(seqs - 1)]
    final = slice((seqs - 1) * span, seqs * span)

    load = block_copies(y_ref, first_row, z, io_sem)
    load_enc = block_copies(enc_ref, 0, enc, enc_sem)
    for copy in load:
        copy.start()
    raws.start(0, raw_src(0, 0))
    load_state(load, z, sums)
    settle_norm(sums, rstd, depth)
    raws.start(1, raw_src(0, 1))

    for layer in range(layers):
        last = layer + 1 == layers
        shift = 10 * layer % 3
        bases = [((6 * layer + g) % 2) * 3 for g in range(7)]

        def raw_slot(idx):
            return (shift + idx) % 3

        def raw_ahead(idx):
            if idx + 2 < 10 or not last:
                raws.start(raw_slot(idx + 2), raw_src(layer, idx + 2))

        def qkv_step(j):
            slot = lax.rem(j + shift, 3)
            raws.wait(slot, raw_src(layer, 0))

            @pl.when(j < 4)
            def _():
                raws.start(lax.rem(j + shift + 2, 3), raw_src(layer, j + 2))

            for later in range(4, 6):

                @pl.when(j == later)
                def _(later=later):
                    raw_ahead(later)

            if layer == 0:
                for turn in range(1, 5):

                    @pl.when(j == turn)
                    def _(turn=turn):
                        for copy in load_enc[(turn - 1) * blocks // 4 : turn * blocks // 4]:
                            copy.start()

            project(big, j * (tile // LANES), xn, slot, tile)

        normalize(z, rstd, xn)
        loop(6, qkv_step)
        if layer == 0:
            ring.start(bases[0], wo_src(0))

        if layer == 0:
            for copy in load_enc:
                copy.wait()

        causal = lax.broadcasted_iota(jnp.int32, (span, span), 1) <= lax.broadcasted_iota(jnp.int32, (span, span), 0)

        def self_step(b):
            slot = lax.rem(b + shift + 6, 3)
            raws.wait(slot, raw_src(layer, 6))
            for later in range(2):

                @pl.when(b == later)
                def _(later=later):
                    raw_ahead(6 + later)

            at = pl.ds(pl.multiple_of(b * span, span), span)
            w = raw[slot].reshape(depth, tile)
            kv_rows = min(512, kv.shape[1])

            def kv_piece(n, m):
                part = slice(m * kv_rows, (m + 1) * kv_rows)
                put_blocks(kv, b * (tile // LANES) + n * piece // LANES, dot(joined(enc, range(blocks), part), w[:, n * piece : (n + 1) * piece]).astype(BF16), part)

            def scores(u):
                return jnp.where(causal, dot_t(big[u, at], big[heads + u, at]), -1e30 / scale)

            def finish(u, probs):
                xn[u, at] = dot(probs, big[2 * heads + u, at]).astype(BF16)

            pieces = [functools.partial(kv_piece, n, m) for n in range(tile // piece) for m in range(kv.shape[1] // kv_rows)]
            attend_units(heads, scores, scale, finish, pieces)

        loop(2, self_step)

        ring.wait(bases[0], wo_src(layer))
        ring.start(bases[1], wc_src(layer))
        for n in range(n_out):
            out_piece(bases[0], n, every)
        settle_norm(sums, rstd, depth)

        def cross_q_step(t):
            slot = lax.rem(t + shift + 8, 3)
            raws.wait(slot, raw_src(layer, 8))
            for later in range(2):

                @pl.when(t == later)
                def _(later=later):
                    raw_ahead(8 + later)

            project(big, t * (tile // LANES), xn, slot, tile)

        normalize(z, rstd, xn)
        loop(2, cross_q_step)

        def cross(b, at, at_kv, filler=()):
            keep = lax.broadcasted_iota(jnp.int32, (1, ctx), 1) < len_ref[b + first_len]

            def scores(g):
                query = jnp.concatenate([big[g * rep + r, at] for r in range(rep)], axis=0)
                return jnp.where(keep, dot_t(query, kv[g, at_kv]), -1e30 / scale)

            def finish(g, probs):
                mixed = dot(probs, kv[kv_heads + g, at_kv]).astype(BF16)
                for r in range(rep):
                    xn[g * rep + r, at] = mixed[r * span : (r + 1) * span]

            attend_units(kv_heads, scores, scale, finish, filler)

        ring.wait(bases[1], wc_src(layer))
        ring.start(bases[2], w1_src(layer, 0))
        for b in range(seqs - 1):
            cross(b, before[b], slice(b * ctx, (b + 1) * ctx))
        pieces = [functools.partial(out_piece, bases[1], n, at) for at in before for n in range(n_out)]
        cross(seqs - 1, final, slice((seqs - 1) * ctx, seqs * ctx), pieces)
        for n in range(n_out):
            out_piece(bases[1], n, final)
        settle_norm(sums, rstd, depth)

        def w1_step(t):
            base = jnp.where(t == 0, bases[2], bases[3])
            ring.wait(base, w1_src(layer, 0))

            @pl.when(t == 0)
            def _():
                ring.start(bases[3], w1_src(layer, 1))

            @pl.when(t == 1)
            def _():
                ring.start(bases[4], w2_src(layer, 0))

            ffn_in(xn, big, ring_buf, base, t, tile, tile, rows // 2)

        normalize(z, rstd, xn)
        loop(2, w1_step)

        def w2_step(t):
            base = jnp.where(t == 0, bases[4], bases[5])
            ring.wait(base, w2_src(layer, 0))

            @pl.when(t == 0)
            def _():
                ring.start(bases[5], w2_src(layer, 1))

            if not last:

                @pl.when(t == 1)
                def _():
                    ring.start(bases[6], wo_src(layer + 1))

            ffn_out(z, sums, big, ring_buf, base, t, tile, piece)

        loop(2, w2_step)
        if not last:
            settle_norm(sums, rstd, depth)

    store = block_copies(out_ref, out_row, z, io_sem, to_hbm=True)
    for copy in store:
        copy.start()
    for copy in store:
        copy.wait()


def decoder_call(first_seq, seqs, y, first_len, enc_len, enc, out_seq, out_seqs, wqkv, wo, wq, wkv, wc, w1, w2):
    span, depth = y.shape[1], y.shape[2]
    layers, ff = wqkv.shape[0], w1.shape[2]
    heads = wqkv.shape[3]
    rows, tile, ctx = seqs * span, depth // 2, enc.shape[0]
    assert ff == 3 * depth and heads * HEAD == depth and seqs == 2
    any_spec = pl.BlockSpec(memory_space=pl.ANY)
    per_layer = 2 * rows * depth * (6 * depth + 2 * ff) + 4 * ctx * depth * depth + 4 * seqs * heads * span * (span + ctx // seqs) * HEAD
    return pl.pallas_call(
        functools.partial(decoder_kernel, first_seq * span, out_seq * span, first_len, seqs, span),
        out_shape=jax.ShapeDtypeStruct((out_seqs * span, depth), BF16),
        in_specs=[pl.BlockSpec(memory_space=pltpu.SMEM)] + [any_spec] * 9,
        out_specs=any_spec,
        scratch_shapes=[
            pltpu.VMEM((depth // LANES, rows, LANES), BF16),
            pltpu.VMEM((depth // LANES, rows, LANES), BF16),
            pltpu.VMEM((ff // LANES, rows, LANES), BF16),
            pltpu.VMEM((depth // LANES, ctx, LANES), BF16),
            pltpu.VMEM((depth // LANES, ctx, LANES), BF16),
            pltpu.VMEM((rows, LANES), F32),
            pltpu.VMEM((rows, LANES), F32),
            pltpu.VMEM((3, depth, tile // HEAD, HEAD), BF16),
            pltpu.VMEM((6, tile // LANES, depth, LANES), BF16),
            pltpu.SemaphoreType.DMA((depth // LANES,)),
            pltpu.SemaphoreType.DMA((depth // LANES,)),
            pltpu.SemaphoreType.DMA((3,)),
            pltpu.SemaphoreType.DMA((6,)),
        ],
        compiler_params=pltpu.CompilerParams(vmem_limit_bytes=VMEM_LIMIT),
        cost_estimate=cost(layers * per_layer, 2 * layers * depth * (8 * depth + 2 * ff)),
        name="decode",
    )(
        enc_len,
        y.reshape(-1, depth),
        enc,
        wqkv,
        wo.reshape(layers, depth, depth),
        wq.reshape(layers, depth, heads, HEAD),
        wkv,
        wc.reshape(layers, depth, depth),
        w1,
        w2,
    )


def solution(mesh):
    stages = mesh.shape["stage"]
    swap = [(source, (source + stages // 2) % stages) for source in range(stages)]
    rows = P(("data", "stage"))
    whole = P()

    def body(x_enc, enc_len, y, enc_wqkv, enc_wo, enc_w1, enc_w2, dec_wqkv, dec_wo, cross_wq, cross_wkv, cross_wo, dec_w1, dec_w2):
        seqs, span, depth = y.shape
        half = seqs // 2
        enc_weights = (enc_wqkv, enc_wo, enc_w1, enc_w2)
        dec_weights = (dec_wqkv, dec_wo, cross_wq, cross_wkv, cross_wo, dec_w1, dec_w2)

        y_recv = lax.ppermute(y, "stage", swap)
        len_recv = lax.ppermute(enc_len, "stage", swap)
        home_enc = encoder_call(half, half, x_enc, enc_len, *enc_weights)
        home_recv = lax.ppermute(home_enc, "stage", swap)
        x_next, _ = lax.optimization_barrier((x_enc, home_enc))
        away_enc = encoder_call(0, half, x_next, enc_len, *enc_weights)
        away_out = decoder_call(0, half, y_recv, 0, enc_len, away_enc, 0, half, *dec_weights)
        out_recv = lax.ppermute(away_out, "stage", swap)
        y_next, _ = lax.optimization_barrier((y, away_out))
        home_out = decoder_call(half, half, y_next, half, len_recv, home_recv, half, seqs, *dec_weights)
        return lax.dynamic_update_slice(home_out, out_recv, (0, 0)).reshape(y.shape)

    return jax.shard_map(body, mesh=mesh, in_specs=(rows, rows, rows) + (whole,) * 11, out_specs=rows, check_vma=False)
```
